128 devices in a mesh: seq: 32 (over x, z, core), tp: 4 (over y).
Axes of the slice: x: 4, y: 4, z: 4, core: 2. Of those that a mesh axis runs over, the one named last changes fastest.
Arguments:
- tokens: bfloat16 [65536, 2560], P('seq'), may hold values from -6 to 6
- w_query: bfloat16 [2560, 512], P(None, 'tp'), may hold values from -0.009765625 to 0.009765625
- w_key: bfloat16 [2560, 512], P(None, 'tp'), may hold values from -0.00048828125 to 0.00048828125
- w_value: bfloat16 [2560, 1024], P(None, 'tp'), may hold values from -0.125 to 0.125
- w_gate: bfloat16 [2560, 512], P(None, 'tp'), may hold values from -0.125 to 0.125
- gate_rate: float32 [512], P('tp'), may hold values from 3.8146973e-06 to 3.0517578e-05
- out_grad: bfloat16 [65536, 1024], P('seq', 'tp'), may hold values from -6 to 6
Outputs:
- input_grad: bfloat16 [65536, 2560], P(('seq', 'tp'))
- gate_signal: float32 [65536, 512], P('seq', 'tp')
The draws below stay inside these ranges and needn't reach their ends.
All inputs are finite; a program needn't handle non-finite values.
Results may differ from the reference program's by a relative error of at most 0.015.
Values sent between devices are 32-bit elements.
A program may use at most 192 MiB of HBM per device.

```python
import math
import jax
import jax.numpy as jnp
from jax import lax

D = 2560
DK = 128
DV = 256
CH = 128
HEADS = 4
TOKENS = 65536


def block_levels(stream_key, extent, split, smallest, high):
    def one(dim, shards_of):
        heights = jax.random.uniform(jax.random.fold_in(jax.random.fold_in(stream_key, 6), dim), (shards_of,), jnp.float32, smallest / len(split), high / len(split))
        return jnp.repeat(jnp.exp(heights), extent[dim] // shards_of).reshape((-1,) + (1,) * (len(extent) - dim - 1))

    gain = one(*split[0])
    for cut in split[1:]:
        gain = gain * one(*cut)
    return gain


def centred(own_key, shape, scale, limit, shards=(), dtype=jnp.bfloat16):
    drawn = scale * jax.random.normal(own_key, shape, jnp.float32)
    if shards:
        drawn = drawn * block_levels(own_key, shape, shards, -0.22, 0.18)
    return jnp.clip(drawn, -limit, limit).astype(dtype)


def setup_inputs(seed: int = 0) -> dict:
    seeds = jax.random.split(jax.random.key(seed), 8)
    return {
        "tokens": centred(seeds[0], (TOKENS, D), 1.0, 6.0, ((0, 32),)),
        "w_query": centred(seeds[1], (D, HEADS * DK), (D * DK) ** -0.5, 0.009765625, ((1, 4),)),
        "w_key": centred(seeds[2], (D, HEADS * DK), (D * TOKENS) ** -0.5, 0.00048828125, ((1, 4),)),
        "w_value": centred(seeds[3], (D, HEADS * DV), D ** -0.5, 0.125, ((1, 4),)),
        "w_gate": centred(seeds[4], (D, HEADS * DK), D ** -0.5, 0.125, ((1, 4),)),
        "gate_rate": jnp.clip(jnp.exp(math.log(3.0517578125e-05) - 2.0794415 * jax.random.uniform(seeds[5], (HEADS * DK,), jnp.float32) ** block_levels(seeds[5], (HEADS * DK,), ((0, 4),), -0.2, 0.2)), 3.814697265625e-06, 3.0517578125e-05),
        "out_grad": centred(seeds[6], (TOKENS, HEADS * DV), 1.0, 6.0, ((0, 32), (1, 4))),
    }


def lower_ones(length):
    places = jnp.arange(length)
    return (places[:, None] >= places[None, :]).astype(jnp.float32)

def low_dot(left, right):
    return jnp.dot(left.astype(jnp.bfloat16), right.astype(jnp.bfloat16), preferred_element_type=jnp.float32)

def run_head(query_rows, key_rows, value_rows, log_gate, initial):
    block_size = CH
    blocks_count = query_rows.shape[0] // block_size
    triangle = lower_ones(block_size)
    pieces = tuple((a.reshape(blocks_count, block_size, a.shape[1]) for a in (query_rows, key_rows, value_rows, log_gate)))

    def advance(memory, piece):
        query_block, key_block, value_block, gate_block = piece
        within = jnp.cumsum(gate_block, axis=0)
        closing = within[-1]
        query_scaled = query_block * jnp.exp(within)
        key_scaled = key_block * jnp.exp(-within)
        scores = low_dot(query_scaled, key_scaled.T) * triangle
        output = low_dot(query_scaled, memory) + low_dot(scores, value_block)
        key_closing = key_block * jnp.exp(closing - within)
        memory = jnp.exp(closing)[:, None] * memory + low_dot(key_closing.T, value_block)
        return (memory, output)
    last_memory, outputs = lax.scan(advance, initial, pieces)
    return (outputs.reshape(-1, outputs.shape[2]), last_memory)

def by_heads(matrix, width):
    return matrix.astype(jnp.float32).reshape(matrix.shape[0], -1, width).transpose(1, 0, 2)

def by_tokens(stacked):
    return stacked.transpose(1, 0, 2).reshape(stacked.shape[1], -1)

def back_project(grad_rows, weight):
    return lax.dot_general(grad_rows, weight, (((1,), (1,)), ((), ())), preferred_element_type=jnp.float32)

def reference(tokens, w_query, w_key, w_value, w_gate, gate_rate, out_grad):
    queries = jnp.dot(tokens, w_query, preferred_element_type=jnp.float32).astype(jnp.bfloat16)
    keys_proj = jnp.dot(tokens, w_key, preferred_element_type=jnp.float32).astype(jnp.bfloat16)
    values_proj = jnp.dot(tokens, w_value, preferred_element_type=jnp.float32).astype(jnp.bfloat16)
    squashed = jax.nn.sigmoid(jnp.dot(tokens, w_gate, preferred_element_type=jnp.float32))
    log_gate = -gate_rate * squashed
    initial = jnp.zeros((HEADS, DK, DV), jnp.float32)

    def forward(query_heads, key_heads, value_heads, gate_heads):
        outputs, last_memory = jax.vmap(run_head)(query_heads, key_heads, value_heads, gate_heads, initial)
        return outputs
    outputs, pullback = jax.vjp(forward, by_heads(queries, DK), by_heads(keys_proj, DK), by_heads(values_proj, DV), by_heads(log_gate, DK))
    grads = pullback(by_heads(out_grad, DV))
    query_grad = by_tokens(grads[0]).astype(jnp.bfloat16)
    key_grad = by_tokens(grads[1]).astype(jnp.bfloat16)
    value_grad = by_tokens(grads[2]).astype(jnp.bfloat16)
    pre_grad = by_tokens(grads[3]) * -gate_rate * squashed * (1.0 - squashed)
    gate_signal = pre_grad * (4.0 * math.sqrt(TOKENS * DK / DV))
    gate_grad = pre_grad.astype(jnp.bfloat16)
    mixed = back_project(query_grad, w_query) + back_project(key_grad, w_key)
    mixed = mixed + back_project(value_grad, w_value) + back_project(gate_grad, w_gate)
    return (mixed.astype(jnp.bfloat16), gate_signal)
```

```python
import functools
import math

import jax
import jax.numpy as jnp
from jax import lax
from jax.experimental import pallas as pl
from jax.experimental.pallas import tpu as pltpu
from jax.sharding import PartitionSpec as P

CH = 128
PAD = 8
VMEM_LIMIT = 66 * 1000 * 1000
F32, BF16 = jnp.float32, jnp.bfloat16


def mm(left, right, dims):
    return lax.dot_general(left, right, (dims, ((), ())), preferred_element_type=F32)


NN = ((1,), (0,))
NT = ((1,), (1,))
TN = ((0,), (0,))


def tri_sum(triangle, rows):
    high = rows.astype(BF16)
    low = (rows - high.astype(F32)).astype(BF16)
    return mm(triangle, high, NN) + mm(triangle, low, NN)


def kernel(
    seq, tp, dk, dv, tile, scale,
    tok, wq, wk, wv, wg, rate_ref, dout_ref,
    grad_ref, sig_ref,
    wall, xbuf, proj, sq_all, w_all, s_all, m_all, cl_all, state, msg, got, rep, back, edge,
    wown, land, landd, g_send, g_recv, gmat,
    w_sem, x_sem, e1_s, e1_r, e2_s, e2_r, y_s, y_r, p1_s, p1_r, p2_s, p2_r, dd_s, dd_r, gs_sem, gr_sem,
):
    me, rank = lax.axis_index("seq"), lax.axis_index("tp")
    length, width, group = dout_ref.shape[0], wall.shape[0], 3 * dk + dv
    blocks, tiles = length // CH, length // tile
    each = blocks // tp
    depth, part = width // seq, dv // seq
    side = math.isqrt(seq // 2)
    core, chip = lax.rem(me, 2), me // 2
    x_at, z_at = chip // side, lax.rem(chip, side)
    offs = (1, 3, 2)
    target = tuple(lax.rem(rank + tp - off, tp) for off in offs)

    def seq_at(dx, dz, on):
        return (lax.rem(x_at + dx, side) * side + lax.rem(z_at + dz, side)) * 2 + on

    def first(d):
        return seq_at((1 - core) * d, core * d, core)

    def second(d):
        return seq_at(core * d, (1 - core) * d, core)

    ahead, behind = (first(1), second(1)), (first(side - 1), second(side - 1))
    partner = me + 1 - 2 * core

    def remote(src, dst, send, recv, axis, to):
        return pltpu.make_async_remote_copy(
            src_ref=src, dst_ref=dst, send_sem=send, recv_sem=recv, device_id={axis: to},
            device_id_type=pl.DeviceIdType.MESH,
        )

    def w_cross(j):
        return remote(wown, land.at[j, 0, 0], y_s.at[j], y_r.at[j], "tp", target[j])

    def w_line(j, n):
        half = depth // 2
        if n == 0:
            a, b, to = land.at[j, 0, 0], land.at[j, 0, 3], ahead[0]
        elif n == 1:
            a, b, to = land.at[j, 0, 0], land.at[j, 0, 1], behind[0]
        elif n == 2:
            rows = pl.ds(0, half)
            a, b, to = land.at[j, 0, 3, rows], land.at[j, 0, 2, rows], ahead[0]
        else:
            rows = pl.ds(half, half)
            a, b, to = land.at[j, 0, 1, rows], land.at[j, 0, 2, rows], behind[0]
        return remote(a, b, p1_s.at[j, n], p1_r.at[j, n], "seq", to)

    def w_plane(j, n):
        a = n % 4
        if n < 4:
            src, dst, to = land.at[j, 0, a], land.at[j, 3, a], ahead[1]
        elif n < 8:
            src, dst, to = land.at[j, 0, a], land.at[j, 1, a], behind[1]
        elif a < 2:
            src, dst, to = land.at[j, 3, a], land.at[j, 2, a], ahead[1]
        else:
            src, dst, to = land.at[j, 1, a], land.at[j, 2, a], behind[1]
        return remote(src, dst, p2_s.at[j, n], p2_r.at[j, n], "seq", to)

    def w_pair(j, b):
        return remote(land.at[j, b], landd.at[j, b], dd_s.at[j, b], dd_r.at[j, b], "seq", partner)

    def gather(j, stage):
        if stage == 0:
            w_cross(j).wait_recv()
            w_line(j, 0).start()
            w_line(j, 1).start()
            w_plane(j, 0).start()
            w_plane(j, 4).start()
        elif stage == 1:
            for n in (0, 1):
                w_line(j, n).wait_recv()
                w_line(j, n + 2).start()
            for a in (3, 1):
                w_plane(j, a).start()
                w_plane(j, 4 + a).start()
        elif stage == 2:
            for n in (2, 3):
                w_line(j, n).wait_recv()
            w_plane(j, 2).start()
            w_plane(j, 6).start()
            w_pair(j, 0).start()
        elif stage == 3:
            for a in (0, 3, 1, 2):
                w_plane(j, a).wait_recv()
                w_plane(j, 4 + a).wait_recv()
                w_plane(j, 8 + a).start()
            w_pair(j, 3).start()
            w_pair(j, 1).start()
        else:
            for a in range(4):
                w_plane(j, 8 + a).wait_recv()
            w_pair(j, 2).start()

    events = iter(EVENTS)

    def pump(count):
        for _ in range(count):
            gather(*next(events))

    def x_copy(t, slot):
        return pltpu.make_async_copy(
            tok.at[pl.ds(pl.multiple_of(t * tile, tile), tile), :], xbuf.at[slot], x_sem.at[slot]
        )

    loads = []
    for n, (w, start, size) in enumerate(
        ((wq, 0, dk), (wk, dk, dk), (wv, 2 * dk, dv), (wg, 2 * dk + dv, dk))
    ):
        loads.append(pltpu.make_async_copy(w, wall.at[:, pl.ds(start, size)], w_sem.at[n]))
    for load in loads:
        load.start()
    x_copy(0, 0).start()

    barrier = pltpu.get_barrier_semaphore()
    for d in range(1, seq):
        pl.semaphore_signal(
            barrier, inc=1, device_id={"seq": lax.rem(me + d, seq)},
            device_id_type=pl.DeviceIdType.MESH,
        )
    for other in target:
        pl.semaphore_signal(
            barrier, inc=1, device_id={"tp": other}, device_id_type=pl.DeviceIdType.MESH
        )

    rows_at = lax.broadcasted_iota(jnp.int32, (CH, CH), 0)
    cols_at = lax.broadcasted_iota(jnp.int32, (CH, CH), 1)
    lower = (rows_at >= cols_at).astype(F32)
    lower_b = lower.astype(BF16)
    upper_b = (rows_at <= cols_at).astype(BF16)
    rate = rate_ref[...]

    state[...] = jnp.zeros_like(state)
    for load in loads:
        load.wait()
    wown[...] = wall[pl.ds(pl.multiple_of(me * depth, 16), depth), 0:group].astype(F32)
    pl.semaphore_wait(barrier, seq + tp - 2)
    for j in range(3):
        w_cross(j).start()

    def project(t, total):
        slot = lax.rem(t, 2)

        @pl.when(t + 1 < tiles)
        def _():
            x_copy(t + 1, 1 - slot).start()

        for at, count in ((2, 2), (4, 2), (6, 2)):
            @pl.when(t == at)
            def _():
                pump(count)

        x_copy(t, slot).wait()
        out = mm(xbuf[slot], wall[:, 0:group], NN)
        base = pl.multiple_of(t * tile, tile)
        proj[pl.ds(base, tile), :] = out[:, : 2 * dk + dv].astype(BF16)
        squashed = jax.nn.sigmoid(out[:, 2 * dk + dv :])
        sq_all[pl.ds(base, tile), :] = squashed
        for j in range(tile // CH):
            part = slice(j * CH, (j + 1) * CH)
            b = t * (tile // CH) + j
            within = tri_sum(lower_b, -rate * squashed[part])
            w_all[pl.ds(pl.multiple_of(base + j * CH, CH), CH), :] = within
            closing = within[CH - 1 : CH]
            cl_all[b] = jnp.broadcast_to(closing, (PAD, dk))
            query = out[part, :dk].astype(BF16).astype(F32)
            key = out[part, dk : 2 * dk].astype(BF16).astype(F32)
            value = out[part, 2 * dk : 2 * dk + dv].astype(BF16)
            dout = dout_ref[pl.ds(pl.multiple_of(base + j * CH, CH), CH), :]
            query_scaled = (query * jnp.exp(within)).astype(BF16)
            key_closing = (key * jnp.exp(closing - within)).astype(BF16)
            entering = state[0]
            s_all[b] = entering
            state[0] = jnp.exp(closing) * entering + mm(value, key_closing, TN)
            fed = mm(dout, query_scaled, TN)
            m_all[b] = fed
            state[1] += jnp.exp(total) * fed
            total = total + closing
        return total

    total = lax.fori_loop(0, tiles, project, jnp.zeros((1, dk), F32))

    msg[:, 0:part, :] = state[0].reshape(seq, part, dk)
    msg[:, part : 2 * part, :] = state[1].reshape(seq, part, dk)
    msg[:, 2 * part :, :] = jnp.broadcast_to(jnp.exp(total)[None], (seq, PAD, dk))

    def scatter(d):
        to = lax.rem(me + d, seq)
        return remote(msg.at[to], got.at[d], e1_s.at[d], e1_r.at[d], "seq", to)

    def collect(d):
        to = lax.rem(me + d, seq)
        return remote(rep.at[to], back.at[me], e2_s.at[d], e2_r.at[d], "seq", to)

    def start_all(copy):
        def run(d, carry):
            copy(d).start()
            return carry

        lax.fori_loop(1, seq, run, 0)

    def wait_all(copy):
        def run(d, carry):
            copy(d).wait()
            return carry

        lax.fori_loop(1, seq, run, 0)

    start_all(scatter)
    got[0] = msg[me]
    pump(2)
    wait_all(scatter)

    def fold_states(p, run):
        it = lax.rem(me + seq - p, seq)
        rep[p, 0:part, :] = run
        return got[it, pl.ds(2 * part, 1), :] * run + got[it, pl.ds(0, part), :]

    def fold_grads(n, run):
        p = seq - 1 - n
        it = lax.rem(me + seq - p, seq)
        rep[p, part:, :] = run
        return got[it, pl.ds(2 * part, 1), :] * run + got[it, pl.ds(part, part), :]

    lax.fori_loop(0, seq, fold_states, jnp.zeros((part, dk), F32))
    lax.fori_loop(0, seq, fold_grads, jnp.zeros((part, dk), F32))
    start_all(collect)
    back[me] = rep[me]
    pump(2)
    wait_all(collect)
    edge[0] = back[:, 0:part, :].reshape(dv, dk)
    edge[1] = back[:, part:, :].reshape(dv, dk)

    def enter(b, so_far):
        s_all[b] = s_all[b] + jnp.exp(so_far) * edge[0]
        return so_far + cl_all[b, 0:1, :]

    lax.fori_loop(0, blocks, enter, jnp.zeros((1, dk), F32))

    def leave(j, carry):
        b = blocks - 1 - j
        fed = m_all[b]
        leaving = edge[1]
        m_all[b] = leaving
        edge[1] = jnp.exp(cl_all[b, 0:1, :]) * leaving + fed
        return carry

    lax.fori_loop(0, blocks, leave, 0)

    def grads(b):
        rows = pl.ds(pl.multiple_of(b * CH, CH), CH)
        query = proj[rows, 0:dk].astype(F32)
        key = proj[rows, dk : 2 * dk].astype(F32)
        value = proj[rows, 2 * dk : 2 * dk + dv]
        within, squashed, dout = w_all[rows, :], sq_all[rows, :], dout_ref[rows, :]
        closing = within[CH - 1 : CH]
        state, leaving = s_all[b], m_all[b]
        grow, shrink, rest = jnp.exp(within), jnp.exp(-within), jnp.exp(closing - within)
        query_f, key_f, close_f = query * grow, key * shrink, key * rest
        query_s, key_s, close_s = query_f.astype(BF16), key_f.astype(BF16), close_f.astype(BF16)
        scores = (mm(query_s, key_s, NT) * lower).astype(BF16)
        d_scores = (mm(dout, value, NT) * lower).astype(BF16)
        leaving_b = leaving.astype(BF16)
        d_query_s = mm(dout, state.astype(BF16), NN) + mm(d_scores, key_s, NN)
        d_key_s = mm(d_scores, query_s, TN)
        d_close = mm(value, leaving_b, NN)
        d_value = mm(scores, dout, TN) + mm(close_s, leaving_b, NT)
        d_query = d_query_s * grow
        d_key = d_key_s * shrink + d_close * rest
        at_close = d_close * close_f
        d_within = d_query_s * query_f - d_key_s * key_f - at_close
        d_closing = jnp.sum(at_close, axis=0, keepdims=True) + jnp.exp(closing) * jnp.sum(
            leaving * state, axis=0, keepdims=True
        )
        d_gate = tri_sum(upper_b, d_within) + d_closing
        pre = d_gate * -rate * squashed * (1.0 - squashed)
        sig_ref[rows, :] = pre * scale
        return d_query, d_key, d_value, pre

    bounds = ((0, dk), (dk, 2 * dk), (2 * dk, 2 * dk + dv), (2 * dk + dv, group))

    def copy_g(j, i):
        return remote(
            g_send.at[j, i], g_recv.at[j, i], gs_sem.at[j, i], gr_sem.at[j, i], "tp", target[j]
        )

    def away(i, carry):
        for j in (2, 0, 1):
            for (lo, hi), grad in zip(bounds, grads(target[j] * each + i)):
                g_send[j, i, :, lo:hi] = grad
            copy_g(j, i).start()
        for at in range(each):
            @pl.when(i == at)
            def _():
                pump(1)
        return carry

    lax.fori_loop(0, each, away, 0)

    def home(i, carry):
        rows = pl.ds(pl.multiple_of(i * CH, CH), CH)
        for (lo, hi), grad in zip(bounds, grads(rank * each + i)):
            gmat[rows, lo:hi] = grad.astype(BF16)
        return carry

    lax.fori_loop(0, each, home, 0)

    def unpack(j):
        for b in range(4):
            w_pair(j, b).wait_recv()

        def run(n, carry):
            b, a = n // 4, lax.rem(n, 4)
            for buffer, on in ((land, core), (landd, 1 - core)):
                origin = seq_at(a * (1 - on) + b * on, a * on + b * (1 - on), on)
                rows = pl.ds(pl.multiple_of(origin * depth, 16), depth)
                wall[rows, (j + 1) * group : (j + 2) * group] = buffer[j, b, a].astype(BF16)
            return carry

        lax.fori_loop(0, 16, run, 0)

    unpack(0)
    unpack(1)
    pump(1)
    unpack(2)

    step = 512 if width % 512 == 0 else width

    def finish(h, carry):
        for i in range(2):
            rows = pl.ds(pl.multiple_of((2 * h + i) * CH, CH), CH)
            for j in range(3):
                copy_g(j, 2 * h + i).wait_recv()
                gmat[rows, (j + 1) * group : (j + 2) * group] = g_recv[j, 2 * h + i].astype(BF16)
        rows = pl.ds(pl.multiple_of(h * 2 * CH, 2 * CH), 2 * CH)
        packed = gmat[rows, :]
        for at in range(0, width, step):
            cols = slice(at, at + step)
            grad_ref[rows, cols] = mm(packed, wall[cols, :], NT).astype(BF16)
        return carry

    lax.fori_loop(0, each // 2, finish, 0)

    for j in range(3):
        w_cross(j).wait_send()
        for n in range(4):
            w_line(j, n).wait_send()
            w_pair(j, n).wait_send()
        for n in range(12):
            w_plane(j, n).wait_send()
        for i in range(each):
            copy_g(j, i).wait_send()


EVENTS = (
    (0, 0), (1, 0), (2, 0), (0, 1), (1, 1), (0, 2), (2, 1), (1, 2), (0, 3), (2, 2),
    (0, 4), (1, 3), (1, 4), (2, 3), (2, 4),
)


def solution(mesh):
    seq, tp = mesh.shape["seq"], mesh.shape["tp"]

    def body(tokens, w_query, w_key, w_value, w_gate, gate_rate, out_grad):
        length, width = tokens.shape
        dk, dv = w_query.shape[1], w_value.shape[1]
        blocks, each = length // CH, length // CH // tp
        tile = 2 * CH
        group = 3 * dk + dv
        scale = 4.0 * math.sqrt(length * seq * dk / dv)
        depth, part = width // seq, dv // seq
        hbm = pl.BlockSpec(memory_space=pl.ANY)
        vmem = pl.BlockSpec(memory_space=pltpu.VMEM)
        dma = pltpu.SemaphoreType.DMA
        return pl.pallas_call(
            functools.partial(kernel, seq, tp, dk, dv, tile, scale),
            out_shape=(
                jax.ShapeDtypeStruct((length // tp, width), BF16),
                jax.ShapeDtypeStruct((length, dk), F32),
            ),
            in_specs=[hbm] * 5 + [vmem] * 2,
            out_specs=(vmem, vmem),
            scratch_shapes=[
                pltpu.VMEM((width, tp * group), BF16),
                pltpu.VMEM((2, tile, width), BF16),
                pltpu.VMEM((length, 2 * dk + dv), BF16),
                pltpu.VMEM((length, dk), F32),
                pltpu.VMEM((length, dk), F32),
                pltpu.VMEM((blocks, dv, dk), F32),
                pltpu.VMEM((blocks, dv, dk), F32),
                pltpu.VMEM((blocks, PAD, dk), F32),
                pltpu.VMEM((2, dv, dk), F32),
                pltpu.VMEM((seq, 2 * part + PAD, dk), F32),
                pltpu.VMEM((seq, 2 * part + PAD, dk), F32),
                pltpu.VMEM((seq, 2 * part, dk), F32),
                pltpu.VMEM((seq, 2 * part, dk), F32),
                pltpu.VMEM((2, dv, dk), F32),
                pltpu.VMEM((depth, group), F32),
                pltpu.VMEM((3, 4, 4, depth, group), F32),
                pltpu.VMEM((3, 4, 4, depth, group), F32),
                pltpu.VMEM((3, each, CH, group), F32),
                pltpu.VMEM((3, each, CH, group), F32),
                pltpu.VMEM((length // tp, tp * group), BF16),
            ]
            + [dma((4,)), dma((2,))]
            + [dma((seq,))] * 4
            + [dma((3,))] * 2
            + [dma((3, 4))] * 2
            + [dma((3, 12))] * 2
            + [dma((3, 4))] * 2
            + [dma((3, each))] * 2,
            compiler_params=pltpu.CompilerParams(
                collective_id=0, has_side_effects=True, vmem_limit_bytes=VMEM_LIMIT
            ),
        )(tokens, w_query, w_key, w_value, w_gate, gate_rate.reshape(1, dk), out_grad)

    placed = (
        P("seq", None),
        P(None, "tp"),
        P(None, "tp"),
        P(None, "tp"),
        P(None, "tp"),
        P("tp"),
        P("seq", "tp"),
    )
    return jax.shard_map(
        body,
        mesh=mesh,
        in_specs=placed,
        out_specs=(P(("seq", "tp"), None), P("seq", "tp")),
        check_vma=False,
    )
```

```python
import functools
import math

import jax
import jax.numpy as jnp
from jax import lax
from jax.experimental import pallas as pl
from jax.experimental.pallas import tpu as pltpu
from jax.sharding import PartitionSpec as P

CH = 128
PAD = 8
VMEM_LIMIT = 67_043_328
F32, BF16 = jnp.float32, jnp.bfloat16


def mm(left, right, dims):
    return lax.dot_general(left, right, (dims, ((), ())), preferred_element_type=F32)


NN = ((1,), (0,))
NT = ((1,), (1,))
TN = ((0,), (0,))


def tri_sum(triangle, rows):
    high = rows.astype(BF16)
    low = (rows - high.astype(F32)).astype(BF16)
    return mm(triangle, high, NN) + mm(triangle, low, NN)


def kernel(
    seq, tp, dk, dv, tile, scale,
    tok, wq, wk, wv, wg, rate_ref, dout_ref,
    grad_ref, sig_ref,
    wall, xbuf, out_a, out_b, proj, sq_all, w_all, s_all, m_all, cl_all, state, msg, got, rep, back, edge,
    wown, land, landd, d_send, d_recv, r_send, r_recv, st_recv, g_send, g_recv, gmat, acc,
    w_sem, x_sem, e1_s, e1_r, e2_s, e2_r, y_s, y_r, p1_s, p1_r, p2_s, p2_r, dd_s, dd_r,
    do_s, do_r, ra_s, ra_r, st_s, st_r, gs_sem, gr_sem, met,
):
    me, rank = lax.axis_index("seq"), lax.axis_index("tp")
    length, width, group = dout_ref.shape[0], wall.shape[0], 3 * dk + dv
    blocks, pairs = length // CH, length // (2 * tile)
    each = blocks // tp
    chunk = each * CH
    depth, part = width // seq, dv // seq
    side = math.isqrt(seq // 2)
    core, chip = lax.rem(me, 2), me // 2
    x_at, z_at = chip // side, lax.rem(chip, side)
    offs = (1, 3, 2)
    target = tuple(lax.rem(rank + tp - off, tp) for off in offs)
    slots = (1, 2, 1)

    def seq_at(dx, dz, on):
        return (lax.rem(x_at + dx, side) * side + lax.rem(z_at + dz, side)) * 2 + on

    def first(d):
        return seq_at((1 - core) * d, core * d, core)

    def second(d):
        return seq_at(core * d, (1 - core) * d, core)

    ahead, behind = (first(1), second(1)), (first(side - 1), second(side - 1))
    partner = me + 1 - 2 * core

    def remote(src, dst, send, recv, axis, to):
        return pltpu.make_async_remote_copy(
            src_ref=src, dst_ref=dst, send_sem=send, recv_sem=recv, device_id={axis: to},
            device_id_type=pl.DeviceIdType.MESH,
        )

    def notify(sem, axis, to):
        pl.semaphore_signal(
            sem, inc=1, device_id={axis: to}, device_id_type=pl.DeviceIdType.MESH
        )

    def w_cross(j):
        return remote(wown, land.at[j, 0, 0], y_s.at[j], y_r.at[j], "tp", target[j])

    def w_line(j, n):
        half = depth // 2
        if n == 0:
            a, b, to = land.at[j, 0, 0], land.at[j, 0, 3], ahead[0]
        elif n == 1:
            a, b, to = land.at[j, 0, 0], land.at[j, 0, 1], behind[0]
        elif n == 2:
            rows = pl.ds(0, half)
            a, b, to = land.at[j, 0, 3, rows], land.at[j, 0, 2, rows], ahead[0]
        else:
            rows = pl.ds(half, half)
            a, b, to = land.at[j, 0, 1, rows], land.at[j, 0, 2, rows], behind[0]
        return remote(a, b, p1_s.at[j, n], p1_r.at[j, n], "seq", to)

    def w_plane(j, n):
        a = n % 4
        if n < 4:
            src, dst, to = land.at[j, 0, a], land.at[j, 3, a], ahead[1]
        elif n < 8:
            src, dst, to = land.at[j, 0, a], land.at[j, 1, a], behind[1]
        elif a < 2:
            src, dst, to = land.at[j, 3, a], land.at[j, 2, a], ahead[1]
        else:
            src, dst, to = land.at[j, 1, a], land.at[j, 2, a], behind[1]
        return remote(src, dst, p2_s.at[j, n], p2_r.at[j, n], "seq", to)

    def w_pair(j, b):
        return remote(land.at[j, b], landd.at[j, b], dd_s.at[j, b], dd_r.at[j, b], "seq", partner)

    def gather(j, stage):
        if stage == 0:
            w_cross(j).wait_recv()
            w_line(j, 0).start()
            w_line(j, 1).start()
            w_plane(j, 0).start()
            w_plane(j, 4).start()
        elif stage == 1:
            for n in (0, 1):
                w_line(j, n).wait_recv()
                w_line(j, n + 2).start()
            for a in (3, 1):
                w_plane(j, a).start()
                w_plane(j, 4 + a).start()
        elif stage == 2:
            for n in (2, 3):
                w_line(j, n).wait_recv()
            w_plane(j, 2).start()
            w_plane(j, 6).start()
            w_pair(j, 0).start()
        elif stage == 3:
            for a in (0, 3, 1, 2):
                w_plane(j, a).wait_recv()
                w_plane(j, 4 + a).wait_recv()
                w_plane(j, 8 + a).start()
            w_pair(j, 3).start()
            w_pair(j, 1).start()
        else:
            for a in range(4):
                w_plane(j, 8 + a).wait_recv()
            w_pair(j, 2).start()

    events = iter(EVENTS)

    def pump(count):
        for _ in range(count):
            gather(*next(events))

    def pump_at(i, counts):
        for at, count in enumerate(counts):
            if count:
                @pl.when(i == at)
                def _():
                    pump(count)

    def x_copy(k, slot):
        return pltpu.make_async_copy(
            tok.at[pl.ds(pl.multiple_of(k * 2 * tile, 2 * tile), 2 * tile), :], xbuf.at[slot],
            x_sem.at[slot],
        )

    def copy_d(j):
        return remote(d_send.at[j], d_recv.at[j], do_s.at[j], do_r.at[j], "tp", target[j])

    def copy_r(j):
        return remote(r_send, r_recv.at[j], ra_s.at[j], ra_r.at[j], "tp", target[j])

    def copy_st(j, n):
        source = (s_all.at[target[j] * each], m_all.at[target[j] * each + each - 1])[n]
        return remote(source, st_recv.at[j, n], st_s.at[j, n], st_r.at[j, n], "tp", target[j])

    def copy_g(i):
        return remote(
            g_send.at[i], g_recv.at[i], gs_sem.at[i], gr_sem.at[i], "tp", target[2]
        )

    loads = []
    for n, (w, start, size) in enumerate(
        ((wq, 0, dk), (wk, dk, dk), (wv, 2 * dk, dv), (wg, 2 * dk + dv, dk))
    ):
        loads.append(pltpu.make_async_copy(w, wall.at[:, pl.ds(start, size)], w_sem.at[n]))
    for load in loads:
        load.start()
    x_copy(0, 0).start()

    barrier = pltpu.get_barrier_semaphore()
    for d in range(1, side):
        notify(barrier, "seq", first(d))
        notify(barrier, "seq", second(d))
    notify(barrier, "seq", partner)
    for to in target:
        notify(barrier, "tp", to)

    rows_at = lax.broadcasted_iota(jnp.int32, (CH, CH), 0)
    cols_at = lax.broadcasted_iota(jnp.int32, (CH, CH), 1)
    lower = (rows_at >= cols_at).astype(F32)
    lower_b = lower.astype(BF16)
    upper_b = (rows_at <= cols_at).astype(BF16)
    own_rate = rate_ref[...]

    state[...] = jnp.zeros_like(state)
    out_b[...] = jnp.zeros_like(out_b)
    r_send[...] = jnp.broadcast_to(own_rate, (PAD, dk))
    for j in range(2):
        rows = pl.ds(pl.multiple_of(target[j] * chunk, chunk), chunk)
        d_send[j] = dout_ref[rows, :].astype(F32)
    for load in loads:
        load.wait()
    wown[...] = wall[pl.ds(pl.multiple_of(me * depth, 16), depth), 0:group].astype(F32)
    pl.semaphore_wait(barrier, 2 * side - 1 + tp - 1)
    for j in range(3):
        w_cross(j).start()
    for j in range(2):
        copy_r(j).start()
        copy_d(j).start()
    for d in range(1, side):
        notify(met.at[0], "seq", first(d))

    def post(out, t, rate, total, dout_at, slope):
        base = pl.multiple_of(t * tile, tile)
        proj[pl.ds(base, tile), :] = out[:, : 2 * dk + dv].astype(BF16)
        squashed = jax.nn.sigmoid(out[:, 2 * dk + dv :])
        sq_all[pl.ds(base, tile), :] = squashed
        for n in range(tile // CH):
            here = slice(n * CH, (n + 1) * CH)
            b = t * (tile // CH) + n
            within = tri_sum(lower_b, -rate * squashed[here])
            rows = pl.ds(pl.multiple_of(base + n * CH, CH), CH)
            w_all[rows, :] = within
            closing = within[CH - 1 : CH]
            cl_all[b] = jnp.broadcast_to(closing, (PAD, dk))
            query = out[here, :dk].astype(BF16).astype(F32)
            key = out[here, dk : 2 * dk].astype(BF16).astype(F32)
            value = out[here, 2 * dk : 2 * dk + dv].astype(BF16)
            query_scaled = (query * jnp.exp(within)).astype(BF16)
            key_closing = (key * jnp.exp(closing - within)).astype(BF16)
            entering = state[0]
            s_all[b] = entering
            state[0] = jnp.exp(closing) * entering + mm(value, key_closing, TN)
            fed = mm(dout_at(rows), query_scaled, TN)
            m_all[b] = fed
            if slope is not None:
                state[1] += jnp.exp(total) * fed
                total = total + slope * closing
        return total

    def own_dout(rows):
        return dout_ref[rows, :]

    def project(k, total):
        slot = lax.rem(k, 2)
        x_copy(k, slot).wait()

        @pl.when(k + 1 < pairs)
        def _():
            x_copy(k + 1, 1 - slot).start()

        pump_at(k, PUMPS_PROJECT)
        out_a[...] = mm(xbuf[slot, 0:tile], wall[:, 0:group], NN)
        total = post(
            out_b, jnp.maximum(2 * k - 1, 0), own_rate, total, own_dout,
            jnp.minimum(k, 1).astype(F32),
        )
        out_b[...] = mm(xbuf[slot, tile : 2 * tile], wall[:, 0:group], NN)
        return post(out_a, 2 * k, own_rate, total, own_dout, 1.0)

    total = lax.fori_loop(0, pairs, project, jnp.zeros((1, dk), F32))
    pl.semaphore_wait(met.at[0], side - 1)
    notify(met.at[1], "seq", partner)
    total = post(out_b, 2 * pairs - 1, own_rate, total, own_dout, 1.0)
    x_copy(rank, 0).start()

    msg[:, 0:part, :] = state[0].reshape(seq, part, dk)
    msg[:, part : 2 * part, :] = state[1].reshape(seq, part, dk)
    msg[:, 2 * part :, :] = jnp.broadcast_to(jnp.exp(total)[None], (seq, PAD, dk))
    pl.semaphore_wait(met.at[1], 1)

    def scatter(d):
        to = lax.rem(me + d, seq)
        return remote(msg.at[to], got.at[d], e1_s.at[d], e1_r.at[d], "seq", to)

    def collect(d):
        to = lax.rem(me + d, seq)
        return remote(rep.at[to], back.at[me], e2_s.at[d], e2_r.at[d], "seq", to)

    def start_all(copy):
        def run(d, carry):
            copy(d).start()
            return carry

        lax.fori_loop(1, seq, run, 0)

    def wait_all(copy):
        def run(d, carry):
            copy(d).wait()
            return carry

        lax.fori_loop(1, seq, run, 0)

    start_all(scatter)
    got[0] = msg[me]
    pump(PUMP_SCATTER)
    wait_all(scatter)

    def fold_states(p, run):
        it = lax.rem(me + seq - p, seq)
        rep[p, 0:part, :] = run
        return got[it, pl.ds(2 * part, 1), :] * run + got[it, pl.ds(0, part), :]

    def fold_grads(n, run):
        p = seq - 1 - n
        it = lax.rem(me + seq - p, seq)
        rep[p, part:, :] = run
        return got[it, pl.ds(2 * part, 1), :] * run + got[it, pl.ds(part, part), :]

    lax.fori_loop(0, seq, fold_states, jnp.zeros((part, dk), F32))
    lax.fori_loop(0, seq, fold_grads, jnp.zeros((part, dk), F32))
    start_all(collect)
    back[me] = rep[me]
    pump(PUMP_COLLECT)
    wait_all(collect)
    edge[0] = back[:, 0:part, :].reshape(dv, dk)
    edge[1] = back[:, part:, :].reshape(dv, dk)

    def enter(b, so_far):
        s_all[b] = s_all[b] + jnp.exp(so_far) * edge[0]
        return so_far + cl_all[b, 0:1, :]

    lax.fori_loop(0, blocks, enter, jnp.zeros((1, dk), F32))

    def leave_from(count):
        def leave(n, carry):
            b = count - 1 - n
            fed = m_all[b]
            leaving = edge[1]
            m_all[b] = leaving
            edge[1] = jnp.exp(cl_all[b, 0:1, :]) * leaving + fed
            return carry

        lax.fori_loop(0, count, leave, 0)

    leave_from(blocks)
    for j in range(2):
        copy_st(j, 0).start()
        copy_st(j, 1).start()

    def grads(b, rate, dout_at, whole):
        rows = pl.ds(pl.multiple_of(b * CH, CH), CH)
        query = proj[rows, 0:dk].astype(F32)
        key = proj[rows, dk : 2 * dk].astype(F32)
        value = proj[rows, 2 * dk : 2 * dk + dv]
        within, squashed, dout = w_all[rows, :], sq_all[rows, :], dout_at(rows)
        closing = within[CH - 1 : CH]
        entering, leaving = s_all[b], m_all[b]
        grow, shrink, rest = jnp.exp(within), jnp.exp(-within), jnp.exp(closing - within)
        query_f, key_f, close_f = query * grow, key * shrink, key * rest
        query_s, key_s, close_s = query_f.astype(BF16), key_f.astype(BF16), close_f.astype(BF16)
        d_scores = (mm(dout, value, NT) * lower).astype(BF16)
        leaving_b = leaving.astype(BF16)
        d_query_s = mm(dout, entering.astype(BF16), NN) + mm(d_scores, key_s, NN)
        d_key_s = mm(d_scores, query_s, TN)
        d_close = mm(value, leaving_b, NN)
        at_close = d_close * close_f
        d_within = d_query_s * query_f - d_key_s * key_f - at_close
        d_closing = jnp.sum(at_close, axis=0, keepdims=True) + jnp.exp(closing) * jnp.sum(
            leaving * entering, axis=0, keepdims=True
        )
        d_gate = tri_sum(upper_b, d_within) + d_closing
        pre = d_gate * -rate * squashed * (1.0 - squashed)
        if not whole:
            return pre
        scores = (mm(query_s, key_s, NT) * lower).astype(BF16)
        d_query = d_query_s * grow
        d_key = d_key_s * shrink + d_close * rest
        d_value = mm(scores, dout, TN) + mm(close_s, leaving_b, NT)
        return d_query, d_key, d_value, pre

    bounds = ((0, dk), (dk, 2 * dk), (2 * dk, 2 * dk + dv), (2 * dk + dv, group))

    def signal_of(b, pre):
        sig_ref[pl.ds(pl.multiple_of(b * CH, CH), CH), :] = pre * scale

    def away(i, carry):
        b = target[2] * each + i
        found = grads(b, own_rate, own_dout, True)
        signal_of(b, found[3])
        for (lo, hi), grad in zip(bounds, found):
            g_send[i, :, lo:hi] = grad
        copy_g(i).start()
        pump_at(i, PUMPS_AWAY)
        return carry

    lax.fori_loop(0, each, away, 0)

    def home(i, carry):
        b = rank * each + i
        found = grads(b, own_rate, own_dout, True)
        signal_of(b, found[3])
        rows = pl.ds(pl.multiple_of(i * CH, CH), CH)
        for (lo, hi), grad in zip(bounds, found):
            gmat[rows, lo:hi] = grad.astype(BF16)
        pump_at(i, PUMPS_HOME)
        return carry

    lax.fori_loop(0, each, home, 0)

    def aside(i, carry):
        for j in range(2):
            b = target[j] * each + i
            signal_of(b, grads(b, own_rate, own_dout, False))
        pump_at(i, PUMPS_ASIDE)
        return carry

    lax.fori_loop(0, each, aside, 0)

    def unpack(j):
        start = slots[j] * group
        for b in range(4):
            w_pair(j, b).wait_recv()

        def run(n, carry):
            b, a = n // 4, lax.rem(n, 4)
            for buffer, on in ((land, core), (landd, 1 - core)):
                origin = seq_at(a * (1 - on) + b * on, a * on + b * (1 - on), on)
                rows = pl.ds(pl.multiple_of(origin * depth, 16), depth)
                wall[rows, start : start + group] = buffer[j, b, a].astype(BF16)
            return carry

        lax.fori_loop(0, 16, run, 0)

    x_copy(rank, 0).wait()
    for j in range(2):
        for n in range(2):
            copy_st(j, n).wait_send()

    def near(j):
        start = slots[j] * group
        unpack(j)
        copy_r(j).wait_recv()
        copy_d(j).wait_recv()
        for n in range(2):
            copy_st(j, n).wait_recv()
        rate = r_recv[j, 0:1, :]

        def dout_at(rows):
            return d_recv[j, rows, :].astype(BF16)

        state[0] = st_recv[j, 0]
        edge[1] = st_recv[j, 1]
        out_a[...] = mm(xbuf[0, 0:tile], wall[:, start : start + group], NN)
        out_b[...] = mm(xbuf[0, tile : 2 * tile], wall[:, start : start + group], NN)
        post(out_a, 0, rate, None, dout_at, None)
        post(out_b, 1, rate, None, dout_at, None)
        leave_from(each)

        def run(i, carry):
            rows = pl.ds(pl.multiple_of(i * CH, CH), CH)
            for (lo, hi), grad in zip(bounds, grads(i, rate, dout_at, True)):
                gmat[rows, (j + 1) * group + lo : (j + 1) * group + hi] = grad.astype(BF16)
            return carry

        lax.fori_loop(0, each, run, 0)

    near(0)
    pump(PUMP_NEAR)
    near(1)

    step = 512 if width % 512 == 0 else width

    def gather_own(n, carry):
        cols = pl.ds(pl.multiple_of(n * step, step), step)
        acc[n] = mm(gmat[...], wall[cols, :], NT)
        return carry

    lax.fori_loop(0, width // step, gather_own, 0)
    for event in events:
        gather(*event)
    unpack(2)
    for i in range(each):
        copy_g(i).wait_recv()
        gmat[i * CH : (i + 1) * CH, 0:group] = g_recv[i].astype(BF16)
    start = slots[2] * group
    for n in range(width // step):
        cols = slice(n * step, (n + 1) * step)
        grad_ref[:, cols] = (
            acc[n] + mm(gmat[:, 0:group], wall[cols, start : start + group], NT)
        ).astype(BF16)

    for j in range(3):
        w_cross(j).wait_send()
        for n in range(4):
            w_line(j, n).wait_send()
            w_pair(j, n).wait_send()
        for n in range(12):
            w_plane(j, n).wait_send()
    for j in range(2):
        copy_r(j).wait_send()
        copy_d(j).wait_send()
    for i in range(each):
        copy_g(i).wait_send()


EVENTS = (
    (0, 0), (1, 0), (2, 0), (0, 1), (1, 1), (2, 1), (0, 2), (1, 2), (2, 2),
    (0, 3), (0, 4), (1, 3), (1, 4), (2, 3), (2, 4),
)
PUMPS_PROJECT = (0, 0, 2, 0)
PUMP_SCATTER = 3
PUMP_COLLECT = 3
PUMPS_AWAY = (0, 0, 1, 1)
PUMPS_HOME = (0, 0, 0, 1)
PUMPS_ASIDE = (0, 0, 0, 1)
PUMP_NEAR = 2


def solution(mesh):
    seq, tp = mesh.shape["seq"], mesh.shape["tp"]

    def body(tokens, w_query, w_key, w_value, w_gate, gate_rate, out_grad):
        length, width = tokens.shape
        dk, dv = w_query.shape[1], w_value.shape[1]
        blocks, each = length // CH, length // CH // tp
        tile = 2 * CH
        group = 3 * dk + dv
        chunk = each * CH
        scale = 4.0 * math.sqrt(length * seq * dk / dv)
        depth, part = width // seq, dv // seq
        step = 512 if width % 512 == 0 else width
        hbm = pl.BlockSpec(memory_space=pl.ANY)
        vmem = pl.BlockSpec(memory_space=pltpu.VMEM)
        dma = pltpu.SemaphoreType.DMA
        return pl.pallas_call(
            functools.partial(kernel, seq, tp, dk, dv, tile, scale),
            out_shape=(
                jax.ShapeDtypeStruct((chunk, width), BF16),
                jax.ShapeDtypeStruct((length, dk), F32),
            ),
            in_specs=[hbm] * 5 + [vmem] * 2,
            out_specs=(vmem, vmem),
            scratch_shapes=[
                pltpu.VMEM((width, 3 * group), BF16),
                pltpu.VMEM((2, 2 * tile, width), BF16),
                pltpu.VMEM((tile, group), F32),
                pltpu.VMEM((tile, group), F32),
                pltpu.VMEM((length, 2 * dk + dv), BF16),
                pltpu.VMEM((length, dk), F32),
                pltpu.VMEM((length, dk), F32),
                pltpu.VMEM((blocks, dv, dk), F32),
                pltpu.VMEM((blocks, dv, dk), F32),
                pltpu.VMEM((blocks, PAD, dk), F32),
                pltpu.VMEM((2, dv, dk), F32),
                pltpu.VMEM((seq, 2 * part + PAD, dk), F32),
                pltpu.VMEM((seq, 2 * part + PAD, dk), F32),
                pltpu.VMEM((seq, 2 * part, dk), F32),
                pltpu.VMEM((seq, 2 * part, dk), F32),
                pltpu.VMEM((2, dv, dk), F32),
                pltpu.VMEM((depth, group), F32),
                pltpu.VMEM((3, 4, 4, depth, group), F32),
                pltpu.VMEM((3, 4, 4, depth, group), F32),
                pltpu.VMEM((2, chunk, dv), F32),
                pltpu.VMEM((2, chunk, dv), F32),
                pltpu.VMEM((PAD, dk), F32),
                pltpu.VMEM((2, PAD, dk), F32),
                pltpu.VMEM((2, 2, dv, dk), F32),
                pltpu.VMEM((each, CH, group), F32),
                pltpu.VMEM((each, CH, group), F32),
                pltpu.VMEM((chunk, 3 * group), BF16),
                pltpu.VMEM((width // step, chunk, step), F32),
            ]
            + [dma((4,)), dma((2,))]
            + [dma((seq,))] * 4
            + [dma((3,))] * 2
            + [dma((3, 4))] * 2
            + [dma((3, 12))] * 2
            + [dma((3, 4))] * 2
            + [dma((2,))] * 4
            + [dma((2, 2))] * 2
            + [dma((each,))] * 2
            + [pltpu.SemaphoreType.REGULAR((2,))],
            compiler_params=pltpu.CompilerParams(
                collective_id=0, has_side_effects=True, vmem_limit_bytes=VMEM_LIMIT
            ),
        )(tokens, w_query, w_key, w_value, w_gate, gate_rate.reshape(1, dk), out_grad)

    placed = (
        P("seq", None),
        P(None, "tp"),
        P(None, "tp"),
        P(None, "tp"),
        P(None, "tp"),
        P("tp"),
        P("seq", "tp"),
    )
    return jax.shard_map(
        body,
        mesh=mesh,
        in_specs=placed,
        out_specs=(P(("seq", "tp"), None), P("seq", "tp")),
        check_vma=False,
    )
```

```python
import functools
import math

import jax
import jax.numpy as jnp
from jax import lax
from jax.experimental import pallas as pl
from jax.experimental.pallas import tpu as pltpu
from jax.sharding import PartitionSpec as P

CH = 128
PAD = 8
VMEM_LIMIT = 67_043_328
F32, BF16 = jnp.float32, jnp.bfloat16


def mm(left, right, dims):
    return lax.dot_general(left, right, (dims, ((), ())), preferred_element_type=F32)


NN = ((1,), (0,))
NT = ((1,), (1,))
TN = ((0,), (0,))


def tri_sum(triangle, rows):
    high = rows.astype(BF16)
    low = (rows - high.astype(F32)).astype(BF16)
    return mm(triangle, high, NN) + mm(triangle, low, NN)


def kernel(
    seq, tp, dk, dv, tile, scale,
    tok, wq, wk, wv, wg, rate_ref, dout_in,
    grad_out, sig_out,
    wall, xbuf, out_a, out_b, dout_ref, sig_ref, grad_ref, proj, sq_all, w_all, s_all, m_all, cl_all,
    proj_n, sq_n, w_n, s_n, m_n, cl_n, state, msg, got, rep, back, edge,
    wown, land, landd, d_send, d_recv, r_send, r_recv, st_recv, gmat, acc,
    w_sem, x_sem, o_sem, e1_s, e1_r, e2_s, e2_r, y_s, y_r, p1_s, p1_r, p2_s, p2_r, dd_s, dd_r,
    do_s, do_r, ra_s, ra_r, st_s, st_r, met,
):
    me, rank = lax.axis_index("seq"), lax.axis_index("tp")
    length, width, group = dout_ref.shape[0], wall.shape[0], 3 * dk + dv
    blocks, pairs = length // CH, length // (2 * tile)
    each = blocks // tp
    chunk = each * CH
    step = 512 if width % 512 == 0 else width
    depth, part = width // seq, dv // seq
    side = math.isqrt(seq // 2)
    core, chip = lax.rem(me, 2), me // 2
    x_at, z_at = chip // side, lax.rem(chip, side)
    offs = (1, 3, 2)
    target = tuple(lax.rem(rank + tp - off, tp) for off in offs)
    slots = (1, 2, 1)
    own = (proj, sq_all, w_all, s_all, m_all, cl_all)
    other = (proj_n, sq_n, w_n, s_n, m_n, cl_n)

    def seq_at(dx, dz, on):
        return (lax.rem(x_at + dx, side) * side + lax.rem(z_at + dz, side)) * 2 + on

    def first(d):
        return seq_at((1 - core) * d, core * d, core)

    def second(d):
        return seq_at(core * d, (1 - core) * d, core)

    ahead, behind = (first(1), second(1)), (first(side - 1), second(side - 1))
    partner = me + 1 - 2 * core

    def remote(src, dst, send, recv, axis, to):
        return pltpu.make_async_remote_copy(
            src_ref=src, dst_ref=dst, send_sem=send, recv_sem=recv, device_id={axis: to},
            device_id_type=pl.DeviceIdType.MESH,
        )

    def notify(sem, axis, to):
        pl.semaphore_signal(
            sem, inc=1, device_id={axis: to}, device_id_type=pl.DeviceIdType.MESH
        )

    def w_cross(j):
        return remote(wown, land.at[j, 0, 0], y_s.at[j], y_r.at[j], "tp", target[j])

    def w_line(j, n):
        half = depth // 2
        if n == 0:
            a, b, to = land.at[j, 0, 0], land.at[j, 0, 3], ahead[0]
        elif n == 1:
            a, b, to = land.at[j, 0, 0], land.at[j, 0, 1], behind[0]
        elif n == 2:
            rows = pl.ds(0, half)
            a, b, to = land.at[j, 0, 3, rows], land.at[j, 0, 2, rows], ahead[0]
        else:
            rows = pl.ds(half, half)
            a, b, to = land.at[j, 0, 1, rows], land.at[j, 0, 2, rows], behind[0]
        return remote(a, b, p1_s.at[j, n], p1_r.at[j, n], "seq", to)

    def w_plane(j, n):
        a = n % 4
        if n < 4:
            src, dst, to = land.at[j, 0, a], land.at[j, 3, a], ahead[1]
        elif n < 8:
            src, dst, to = land.at[j, 0, a], land.at[j, 1, a], behind[1]
        elif a < 2:
            src, dst, to = land.at[j, 3, a], land.at[j, 2, a], ahead[1]
        else:
            src, dst, to = land.at[j, 1, a], land.at[j, 2, a], behind[1]
        return remote(src, dst, p2_s.at[j, n], p2_r.at[j, n], "seq", to)

    def w_pair(j, b):
        return remote(land.at[j, b], landd.at[j, b], dd_s.at[j, b], dd_r.at[j, b], "seq", partner)

    def gather(j, stage):
        if stage == 0:
            w_cross(j).wait_recv()
            w_line(j, 0).start()
            w_line(j, 1).start()
            w_plane(j, 0).start()
            w_plane(j, 4).start()
        elif stage == 1:
            for n in (0, 1):
                w_line(j, n).wait_recv()
                w_line(j, n + 2).start()
            for a in (3, 1):
                w_plane(j, a).start()
                w_plane(j, 4 + a).start()
        elif stage == 2:
            for n in (2, 3):
                w_line(j, n).wait_recv()
            w_plane(j, 2).start()
            w_plane(j, 6).start()
            w_pair(j, 0).start()
        elif stage == 3:
            for a in (0, 3):
                w_plane(j, a).wait_recv()
                w_plane(j, 4 + a).wait_recv()
                w_plane(j, 8 + a).start()
        elif stage == 4:
            for a in (1, 2):
                w_plane(j, a).wait_recv()
                w_plane(j, 4 + a).wait_recv()
                w_plane(j, 8 + a).start()
            w_pair(j, 3).start()
            w_pair(j, 1).start()
        elif stage == 5:
            for a in range(4):
                w_plane(j, 8 + a).wait_recv()
            w_pair(j, 2).start()
        elif stage == 6:
            w_cross(j).start()
        else:
            copy_d(j).start()

    def x_copy(k, slot):
        return pltpu.make_async_copy(
            tok.at[pl.ds(pl.multiple_of(k * 2 * tile, 2 * tile), 2 * tile), :], xbuf.at[slot],
            x_sem.at[slot],
        )

    def copy_d(j):
        return remote(d_send.at[j], d_recv.at[j], do_s.at[j], do_r.at[j], "tp", target[j])

    def copy_r(j):
        return remote(r_send, r_recv.at[j], ra_s.at[j], ra_r.at[j], "tp", target[j])

    def copy_st(j, n):
        source = (s_all.at[target[j] * each], m_all.at[target[j] * each + each - 1])[n]
        return remote(source, st_recv.at[j, n], st_s.at[j, n], st_r.at[j, n], "tp", target[j])

    def copy_sig(i):
        rows = pl.ds(pl.multiple_of(i * chunk, chunk), chunk)
        return pltpu.make_async_copy(sig_ref.at[rows], sig_out.at[rows], o_sem.at[i])

    def copy_grad(n):
        cols = pl.ds(n * step, step)
        return pltpu.make_async_copy(grad_ref.at[:, cols], grad_out.at[:, cols], o_sem.at[tp + n])

    loads = []
    for n, (w, start, size) in enumerate(
        ((wq, 0, dk), (wk, dk, dk), (wv, 2 * dk, dv), (wg, 2 * dk + dv, dk))
    ):
        loads.append(pltpu.make_async_copy(w, wall.at[:, pl.ds(start, size)], w_sem.at[n]))
    for load in loads:
        load.start()
    dout_load = pltpu.make_async_copy(dout_in, dout_ref, w_sem.at[4])
    dout_load.start()
    x_copy(0, 0).start()

    barrier = pltpu.get_barrier_semaphore()
    for d in range(1, side):
        notify(barrier, "seq", first(d))
        notify(barrier, "seq", second(d))
    notify(barrier, "seq", partner)
    for to in target:
        notify(barrier, "tp", to)

    rows_at = lax.broadcasted_iota(jnp.int32, (CH, CH), 0)
    cols_at = lax.broadcasted_iota(jnp.int32, (CH, CH), 1)
    lower = (rows_at >= cols_at).astype(F32)
    lower_b = lower.astype(BF16)
    upper_b = (rows_at <= cols_at).astype(BF16)
    own_rate = rate_ref[...]

    state[...] = jnp.zeros_like(state)
    out_b[...] = jnp.zeros_like(out_b)
    r_send[...] = jnp.broadcast_to(own_rate, (PAD, dk))
    for load in loads:
        load.wait()
    wown[...] = wall[pl.ds(pl.multiple_of(me * depth, 16), depth), 0:group].astype(F32)
    pl.semaphore_wait(barrier, 2 * side - 1 + tp - 1)
    for j in range(2):
        w_cross(j).start()
    for j in range(3):
        copy_r(j).start()
    for d in range(1, side):
        notify(met.at[0], "seq", first(d))
    dout_load.wait()
    for j in range(3):
        rows = pl.ds(pl.multiple_of(target[j] * chunk, chunk), chunk)
        d_send[j] = dout_ref[rows, :].astype(F32)

    def post(out, t, kept, rate, total, dout_at, slope):
        proj, sq_all, w_all, s_all, m_all, cl_all = kept
        base = pl.multiple_of(t * tile, tile)
        proj[pl.ds(base, tile), :] = out[:, : 2 * dk + dv].astype(BF16)
        squashed = jax.nn.sigmoid(out[:, 2 * dk + dv :])
        sq_all[pl.ds(base, tile), :] = squashed
        for n in range(tile // CH):
            here = slice(n * CH, (n + 1) * CH)
            b = t * (tile // CH) + n
            within = tri_sum(lower_b, -rate * squashed[here])
            rows = pl.ds(pl.multiple_of(base + n * CH, CH), CH)
            w_all[rows, :] = within
            closing = within[CH - 1 : CH]
            cl_all[b] = jnp.broadcast_to(closing, (PAD, dk))
            query = out[here, :dk].astype(BF16).astype(F32)
            key = out[here, dk : 2 * dk].astype(BF16).astype(F32)
            value = out[here, 2 * dk : 2 * dk + dv].astype(BF16)
            query_scaled = (query * jnp.exp(within)).astype(BF16)
            key_closing = (key * jnp.exp(closing - within)).astype(BF16)
            entering = state[0]
            s_all[b] = entering
            state[0] = jnp.exp(closing) * entering + mm(value, key_closing, TN)
            fed = mm(dout_at(rows), query_scaled, TN)
            m_all[b] = fed
            if slope is not None:
                state[1] += jnp.exp(total) * fed
                total = total + slope * closing
        return total

    def own_dout(rows):
        return dout_ref[rows, :]

    def project(k, total):
        slot = lax.rem(k, 2)
        x_copy(k, slot).wait()

        @pl.when(k + 1 < pairs)
        def _():
            x_copy(k + 1, 1 - slot).start()

        for at, *event in EARLY:
            @pl.when(k == at)
            def _():
                gather(*event)

        out_a[...] = mm(xbuf[slot, 0:tile], wall[:, 0:group], NN)
        total = post(
            out_b, jnp.maximum(2 * k - 1, 0), own, own_rate, total, own_dout,
            jnp.minimum(k, 1).astype(F32),
        )
        out_b[...] = mm(xbuf[slot, tile : 2 * tile], wall[:, 0:group], NN)
        return post(out_a, 2 * k, own, own_rate, total, own_dout, 1.0)

    total = lax.fori_loop(0, pairs, project, jnp.zeros((1, dk), F32))
    pl.semaphore_wait(met.at[0], side - 1)
    notify(met.at[1], "seq", partner)
    total = post(out_b, 2 * pairs - 1, own, own_rate, total, own_dout, 1.0)
    x_copy(rank, 0).start()

    msg[:, 0:part, :] = state[0].reshape(seq, part, dk)
    msg[:, part : 2 * part, :] = state[1].reshape(seq, part, dk)
    msg[:, 2 * part :, :] = jnp.broadcast_to(jnp.exp(total)[None], (seq, PAD, dk))
    pl.semaphore_wait(met.at[1], 1)

    def enter_leave(kept, count):
        s_all, m_all, cl_all = kept[3:]

        def enter(b, so_far):
            s_all[b] = s_all[b] + jnp.exp(so_far) * edge[0]
            return so_far + cl_all[b, 0:1, :]

        def leave(n, carry):
            b = count - 1 - n
            fed = m_all[b]
            leaving = edge[1]
            m_all[b] = leaving
            edge[1] = jnp.exp(cl_all[b, 0:1, :]) * leaving + fed
            return carry

        lax.fori_loop(0, count, enter, jnp.zeros((1, dk), F32))
        lax.fori_loop(0, count, leave, 0)

    def grads(b, kept, rate, dout_at, whole):
        proj, sq_all, w_all, s_all, m_all, cl_all = kept
        rows = pl.ds(pl.multiple_of(b * CH, CH), CH)
        query = proj[rows, 0:dk].astype(F32)
        key = proj[rows, dk : 2 * dk].astype(F32)
        value = proj[rows, 2 * dk : 2 * dk + dv]
        within, squashed, dout = w_all[rows, :], sq_all[rows, :], dout_at(rows)
        closing = within[CH - 1 : CH]
        entering, leaving = s_all[b], m_all[b]
        grow, shrink, rest = jnp.exp(within), jnp.exp(-within), jnp.exp(closing - within)
        query_f, key_f, close_f = query * grow, key * shrink, key * rest
        query_s, key_s, close_s = query_f.astype(BF16), key_f.astype(BF16), close_f.astype(BF16)
        d_scores = (mm(dout, value, NT) * lower).astype(BF16)
        leaving_b = leaving.astype(BF16)
        d_query_s = mm(dout, entering.astype(BF16), NN) + mm(d_scores, key_s, NN)
        d_key_s = mm(d_scores, query_s, TN)
        d_close = mm(value, leaving_b, NN)
        at_close = d_close * close_f
        d_within = d_query_s * query_f - d_key_s * key_f - at_close
        d_closing = jnp.sum(at_close, axis=0, keepdims=True) + jnp.exp(closing) * jnp.sum(
            leaving * entering, axis=0, keepdims=True
        )
        d_gate = tri_sum(upper_b, d_within) + d_closing
        pre = d_gate * -rate * squashed * (1.0 - squashed)
        if not whole:
            return pre
        scores = (mm(query_s, key_s, NT) * lower).astype(BF16)
        d_query = d_query_s * grow
        d_key = d_key_s * shrink + d_close * rest
        d_value = mm(scores, dout, TN) + mm(close_s, leaving_b, NT)
        return d_query, d_key, d_value, pre

    bounds = ((0, dk), (dk, 2 * dk), (2 * dk, 2 * dk + dv), (2 * dk + dv, group))

    def unpack(j):
        start = slots[j] * group
        for b in range(4):
            w_pair(j, b).wait_recv()

        def run(n, carry):
            b, a = n // 4, lax.rem(n, 4)
            for buffer, on in ((land, core), (landd, 1 - core)):
                origin = seq_at(a * (1 - on) + b * on, a * on + b * (1 - on), on)
                rows = pl.ds(pl.multiple_of(origin * depth, 16), depth)
                wall[rows, start : start + group] = buffer[j, b, a].astype(BF16)
            return carry

        lax.fori_loop(0, 16, run, 0)

    def near(j):
        start = slots[j] * group
        def dout_at(rows):
            return d_recv[j, rows, :].astype(BF16)

        def before():
            unpack(j)
            state[0] = jnp.zeros((dv, dk), F32)
            out_a[...] = mm(xbuf[0, 0:tile], wall[:, start : start + group], NN)
            out_b[...] = mm(xbuf[0, tile : 2 * tile], wall[:, start : start + group], NN)
            rate = r_recv[j, 0:1, :]
            post(out_a, 0, other, rate, None, dout_at, None)
            post(out_b, 1, other, rate, None, dout_at, None)

        def run(i, carry):
            rows = pl.ds(pl.multiple_of(i * CH, CH), CH)
            found = grads(i, other, r_recv[j, 0:1, :], dout_at, True)
            for (lo, hi), grad in zip(bounds, found):
                gmat[rows, slots[j] * group + lo : slots[j] * group + hi] = grad.astype(BF16)
            return carry

        def after():
            for n in range(2):
                copy_st(j, n).wait_recv()
            edge[0] = st_recv[j, 0]
            edge[1] = st_recv[j, 1]
            enter_leave(other, each)
            lax.fori_loop(0, each, run, 0)

        return before, after

    def arrived(j):
        copy_r(j).wait_recv()
        copy_d(j).wait_recv()

    def scatter(d):
        to = lax.rem(me + d, seq)
        return remote(msg.at[to], got.at[d], e1_s.at[d], e1_r.at[d], "seq", to)

    def collect(d):
        to = lax.rem(me + d, seq)
        return remote(rep.at[to], back.at[me], e2_s.at[d], e2_r.at[d], "seq", to)

    def start_all(copy):
        def run(d, carry):
            copy(d).start()
            return carry

        lax.fori_loop(1, seq, run, 0)

    def wait_all(copy):
        def run(d, carry):
            copy(d).wait()
            return carry

        lax.fori_loop(1, seq, run, 0)

    def fold_states(p, run):
        it = lax.rem(me + seq - p, seq)
        rep[p, 0:part, :] = run
        return got[it, pl.ds(2 * part, 1), :] * run + got[it, pl.ds(0, part), :]

    def fold_grads(n, run):
        p = seq - 1 - n
        it = lax.rem(me + seq - p, seq)
        rep[p, part:, :] = run
        return got[it, pl.ds(2 * part, 1), :] * run + got[it, pl.ds(part, part), :]

    def scatter_start():
        start_all(scatter)
        got[0] = msg[me]

    def fold():
        wait_all(scatter)
        lax.fori_loop(0, seq, fold_states, jnp.zeros((part, dk), F32))
        lax.fori_loop(0, seq, fold_grads, jnp.zeros((part, dk), F32))
        start_all(collect)
        back[me] = rep[me]

    def own_states():
        wait_all(collect)
        edge[0] = back[:, 0:part, :].reshape(dv, dk)
        edge[1] = back[:, part:, :].reshape(dv, dk)
        enter_leave(own, blocks)
        for j in range(3):
            copy_st(j, 0).start()
            copy_st(j, 1).start()

    def signal_of(b, pre):
        sig_ref[pl.ds(pl.multiple_of(b * CH, CH), CH), :] = pre * scale

    def home(i, carry):
        b = rank * each + i
        found = grads(b, own, own_rate, own_dout, True)
        signal_of(b, found[3])
        rows = pl.ds(pl.multiple_of(i * CH, CH), CH)
        for (lo, hi), grad in zip(bounds, found):
            gmat[rows, lo:hi] = grad.astype(BF16)
        return carry

    def aside(i, carry):
        for j in range(3):
            b = target[j] * each + i
            signal_of(b, grads(b, own, own_rate, own_dout, False))
        return carry

    def gather_own(n, carry):
        cols = pl.ds(pl.multiple_of(n * step, step), step)
        acc[n] = mm(gmat[...], wall[cols, :], NT)
        return carry

    def signals_out():
        for i in range(tp):
            copy_sig(i).start()

    def own_chunk():
        x_copy(rank, 0).wait()

    heads = [near(j) for j in range(3)]
    steps = {
        "scatter": scatter_start, "fold": fold, "states": own_states, "chunk": own_chunk,
        "signals": signals_out,
        "home": lambda lo, hi: lax.fori_loop(lo, hi, home, 0),
        "aside": lambda lo, hi: lax.fori_loop(lo, hi, aside, 0),
        "before": lambda j: (arrived(j), heads[j][0]()),
        "after": lambda j: heads[j][1](),
        "backproject": lambda: lax.fori_loop(0, width // step, gather_own, 0),
        "gather": gather,
    }
    for name, *args in PLAN:
        steps[name](*args)
    at = slots[2] * group
    for n in range(width // step):
        cols = slice(n * step, (n + 1) * step)
        grad_ref[:, cols] = (
            acc[n] + mm(gmat[:, at : at + group], wall[cols, at : at + group], NT)
        ).astype(BF16)
        copy_grad(n).start()

    for j in range(3):
        w_cross(j).wait_send()
        copy_r(j).wait_send()
        copy_d(j).wait_send()
        for n in range(2):
            copy_st(j, n).wait_send()
        for n in range(4):
            w_line(j, n).wait_send()
            w_pair(j, n).wait_send()
        for n in range(12):
            w_plane(j, n).wait_send()
    for i in range(tp):
        copy_sig(i).wait()
    for n in range(width // step):
        copy_grad(n).wait()


EARLY = ((2, 0, 0), (3, 1, 0))
PLAN = (
    ("scatter",), ("gather", 0, 1), ("gather", 0, 7), ("gather", 1, 7), ("gather", 2, 6),
    ("gather", 0, 2), ("fold",),
    ("gather", 0, 3), ("gather", 0, 4), ("gather", 1, 1), ("gather", 2, 7), ("chunk",),
    ("gather", 1, 2), ("gather", 1, 3), ("gather", 2, 0), ("gather", 0, 5),
    ("before", 0), ("gather", 1, 4), ("gather", 2, 1), ("states",),
    ("home", 0, 2), ("gather", 1, 5), ("home", 2, 4), ("gather", 2, 2),
    ("after", 0), ("gather", 2, 3), ("before", 1), ("gather", 2, 4), ("after", 1),
    ("aside", 0, 2), ("gather", 2, 5), ("aside", 2, 4), ("signals",),
    ("backproject",), ("before", 2), ("after", 2),
)


def solution(mesh):
    seq, tp = mesh.shape["seq"], mesh.shape["tp"]

    def body(tokens, w_query, w_key, w_value, w_gate, gate_rate, out_grad):
        length, width = tokens.shape
        dk, dv = w_query.shape[1], w_value.shape[1]
        blocks, each = length // CH, length // CH // tp
        tile = 2 * CH
        group = 3 * dk + dv
        chunk = each * CH
        scale = 4.0 * math.sqrt(length * seq * dk / dv)
        depth, part = width // seq, dv // seq
        step = 512 if width % 512 == 0 else width
        hbm = pl.BlockSpec(memory_space=pl.ANY)
        vmem = pl.BlockSpec(memory_space=pltpu.VMEM)
        dma = pltpu.SemaphoreType.DMA
        return pl.pallas_call(
            functools.partial(kernel, seq, tp, dk, dv, tile, scale),
            out_shape=(
                jax.ShapeDtypeStruct((chunk, width), BF16),
                jax.ShapeDtypeStruct((length, dk), F32),
            ),
            in_specs=[hbm] * 5 + [vmem, hbm],
            out_specs=(hbm, hbm),
            scratch_shapes=[
                pltpu.VMEM((width, 3 * group), BF16),
                pltpu.VMEM((2, 2 * tile, width), BF16),
                pltpu.VMEM((tile, group), F32),
                pltpu.VMEM((tile, group), F32),
                pltpu.VMEM((length, dv), BF16),
                pltpu.VMEM((length, dk), F32),
                pltpu.VMEM((chunk, width), BF16),
                pltpu.VMEM((length, 2 * dk + dv), BF16),
                pltpu.VMEM((length, dk), F32),
                pltpu.VMEM((length, dk), F32),
                pltpu.VMEM((blocks, dv, dk), F32),
                pltpu.VMEM((blocks, dv, dk), F32),
                pltpu.VMEM((blocks, PAD, dk), F32),
                pltpu.VMEM((chunk, 2 * dk + dv), BF16),
                pltpu.VMEM((chunk, dk), F32),
                pltpu.VMEM((chunk, dk), F32),
                pltpu.VMEM((each, dv, dk), F32),
                pltpu.VMEM((each, dv, dk), F32),
                pltpu.VMEM((each, PAD, dk), F32),
                pltpu.VMEM((2, dv, dk), F32),
                pltpu.VMEM((seq, 2 * part + PAD, dk), F32),
                pltpu.VMEM((seq, 2 * part + PAD, dk), F32),
                pltpu.VMEM((seq, 2 * part, dk), F32),
                pltpu.VMEM((seq, 2 * part, dk), F32),
                pltpu.VMEM((2, dv, dk), F32),
                pltpu.VMEM((depth, group), F32),
                pltpu.VMEM((3, 4, 4, depth, group), F32),
                pltpu.VMEM((3, 4, 4, depth, group), F32),
                pltpu.VMEM((3, chunk, dv), F32),
                pltpu.VMEM((3, chunk, dv), F32),
                pltpu.VMEM((PAD, dk), F32),
                pltpu.VMEM((3, PAD, dk), F32),
                pltpu.VMEM((3, 2, dv, dk), F32),
                pltpu.VMEM((chunk, 3 * group), BF16),
                pltpu.VMEM((width // step, chunk, step), F32),
            ]
            + [dma((5,)), dma((2,)), dma((tp + width // step,))]
            + [dma((seq,))] * 4
            + [dma((3,))] * 2
            + [dma((3, 4))] * 2
            + [dma((3, 12))] * 2
            + [dma((3, 4))] * 2
            + [dma((3,))] * 4
            + [dma((3, 2))] * 2
            + [pltpu.SemaphoreType.REGULAR((2,))],
            compiler_params=pltpu.CompilerParams(
                collective_id=0, has_side_effects=True, vmem_limit_bytes=VMEM_LIMIT
            ),
        )(tokens, w_query, w_key, w_value, w_gate, gate_rate.reshape(1, dk), out_grad)

    placed = (
        P("seq", None),
        P(None, "tp"),
        P(None, "tp"),
        P(None, "tp"),
        P(None, "tp"),
        P("tp"),
        P("seq", "tp"),
    )
    return jax.shard_map(
        body,
        mesh=mesh,
        in_specs=placed,
        out_specs=(P(("seq", "tp"), None), P("seq", "tp")),
        check_vma=False,
    )
```

```python
import functools
import math

import jax
import jax.numpy as jnp
from jax import lax
from jax.experimental import pallas as pl
from jax.experimental.pallas import tpu as pltpu
from jax.sharding import PartitionSpec as P

CH = 128
PAD = 8
VMEM_LIMIT = 63_200_000
F32, BF16 = jnp.float32, jnp.bfloat16


def mm(left, right, dims):
    return lax.dot_general(left, right, (dims, ((), ())), preferred_element_type=F32)


NN = ((1,), (0,))
NT = ((1,), (1,))
TN = ((0,), (0,))


def tri_sum(triangle, rows):
    high = rows.astype(BF16)
    low = (rows - high.astype(F32)).astype(BF16)
    return mm(triangle, high, NN) + mm(triangle, low, NN)


def kernel(
    seq, tp, dk, dv, tile, scale,
    tok, wq, wk, wv, wg, rate_ref, dout_in,
    grad_ref, sig_ref,
    wall, xbuf, out_a, out_b, dout_ref, proj, sq_all, w_all, s_all, m_all, cl_all,
    proj_n, sq_n, w_n, s_n, m_n, cl_n, state, msg, got, rep, back, edge,
    wown, wmore, land, landd, d_send, d_recv, r_send, r_recv, st_recv, gmat, acc,
    w_sem, x_sem, e1_s, e1_r, e2_s, e2_r, y_s, y_r, ym_s, ym_r, p1_s, p1_r, p2_s, p2_r, dd_s, dd_r,
    do_s, do_r, ra_s, ra_r, st_s, st_r, met,
):
    me, rank = lax.axis_index("seq"), lax.axis_index("tp")
    length, width, group = dout_ref.shape[0], wall.shape[0], 3 * dk + dv
    blocks, pairs = length // CH, length // (2 * tile)
    each = blocks // tp
    chunk = each * CH
    step = 512 if width % 512 == 0 else width
    depth, part = width // seq, dv // seq
    side = math.isqrt(seq // 2)
    core, chip = lax.rem(me, 2), me // 2
    x_at, z_at = chip // side, lax.rem(chip, side)
    offs = (1, 3, 2)
    target = tuple(lax.rem(rank + tp - off, tp) for off in offs)
    slots = (1, 2, 1)
    own = (proj, sq_all, w_all, s_all, m_all, cl_all)
    other = (proj_n, sq_n, w_n, s_n, m_n, cl_n)

    def seq_at(dx, dz, on):
        return (lax.rem(x_at + dx, side) * side + lax.rem(z_at + dz, side)) * 2 + on

    def first(d):
        return seq_at((1 - core) * d, core * d, core)

    def second(d):
        return seq_at(core * d, (1 - core) * d, core)

    ahead, behind = (first(1), second(1)), (first(side - 1), second(side - 1))
    partner = me + 1 - 2 * core

    def remote(src, dst, send, recv, axis, to):
        return pltpu.make_async_remote_copy(
            src_ref=src, dst_ref=dst, send_sem=send, recv_sem=recv, device_id={axis: to},
            device_id_type=pl.DeviceIdType.MESH,
        )

    def notify(sem, axis, to):
        pl.semaphore_signal(
            sem, inc=1, device_id={axis: to}, device_id_type=pl.DeviceIdType.MESH
        )

    def w_cross(j):
        return remote(wown, land.at[j, 0, 0], y_s.at[j], y_r.at[j], "tp", target[j])

    def w_more(j, n):
        a = 3 * n
        return remote(
            wmore.at[n], land.at[j, 2, a], ym_s.at[j, n], ym_r.at[j, n], "tp", target[j]
        )

    def w_line(j, n):
        half = depth // 2
        if n == 0:
            a, b, to = land.at[j, 0, 0], land.at[j, 0, 3], ahead[0]
        elif n == 1:
            a, b, to = land.at[j, 0, 0], land.at[j, 0, 1], behind[0]
        elif n == 2:
            rows = pl.ds(0, half)
            a, b, to = land.at[j, 0, 3, rows], land.at[j, 0, 2, rows], ahead[0]
        else:
            rows = pl.ds(half, half)
            a, b, to = land.at[j, 0, 1, rows], land.at[j, 0, 2, rows], behind[0]
        return remote(a, b, p1_s.at[j, n], p1_r.at[j, n], "seq", to)

    def w_plane(j, n):
        a = n % 4
        if n < 4:
            src, dst, to = land.at[j, 0, a], land.at[j, 3, a], ahead[1]
        elif n < 8:
            src, dst, to = land.at[j, 0, a], land.at[j, 1, a], behind[1]
        elif a < 2:
            src, dst, to = land.at[j, 3, a], land.at[j, 2, a], ahead[1]
        else:
            src, dst, to = land.at[j, 1, a], land.at[j, 2, a], behind[1]
        return remote(src, dst, p2_s.at[j, n], p2_r.at[j, n], "seq", to)

    def w_pair(j, b):
        return remote(land.at[j, b], landd.at[j, b], dd_s.at[j, b], dd_r.at[j, b], "seq", partner)

    def gather(j, stage):
        if stage == 0:
            w_cross(j).wait_recv()
            w_line(j, 0).start()
            w_line(j, 1).start()
            w_plane(j, 0).start()
            w_plane(j, 4).start()
        elif stage == 1:
            for n in (0, 1):
                w_line(j, n).wait_recv()
                w_line(j, n + 2).start()
            for a in (3, 1):
                w_plane(j, a).start()
                w_plane(j, 4 + a).start()
        elif stage == 2:
            for n in (2, 3):
                w_line(j, n).wait_recv()
            w_plane(j, 2).start()
            w_plane(j, 6).start()
            w_pair(j, 0).start()
        elif stage == 3:
            for a in (0, 3):
                w_plane(j, a).wait_recv()
                w_plane(j, 4 + a).wait_recv()
                if j == 2:
                    w_plane(j, 8 + a).start()
        elif stage == 4:
            for a in (1, 2):
                w_plane(j, a).wait_recv()
                w_plane(j, 4 + a).wait_recv()
                w_plane(j, 8 + a).start()
            w_pair(j, 3).start()
            w_pair(j, 1).start()
        elif stage == 5:
            for n in range(2):
                if j == 2:
                    w_plane(j, 8 + 3 * n).wait_recv()
                else:
                    w_more(j, n).wait_recv()
                w_plane(j, 9 + n).wait_recv()
            w_pair(j, 2).start()
        elif stage == 8:
            w_more(j, 0).start()
            w_more(j, 1).start()
        elif stage == 6:
            w_cross(j).start()
        else:
            copy_d(j).start()

    def x_copy(k, slot):
        return pltpu.make_async_copy(
            tok.at[pl.ds(pl.multiple_of(k * 2 * tile, 2 * tile), 2 * tile), :], xbuf.at[slot],
            x_sem.at[slot],
        )

    def copy_d(j):
        return remote(d_send.at[j], d_recv.at[j], do_s.at[j], do_r.at[j], "tp", target[j])

    def copy_r(j):
        return remote(r_send, r_recv.at[j], ra_s.at[j], ra_r.at[j], "tp", target[j])

    def copy_st(j, n):
        source = (s_all.at[target[j] * each], m_all.at[target[j] * each + each - 1])[n]
        return remote(source, st_recv.at[j, n], st_s.at[j, n], st_r.at[j, n], "tp", target[j])

    loads = []
    for n, (w, start, size) in enumerate(
        ((wq, 0, dk), (wk, dk, dk), (wv, 2 * dk, dv), (wg, 2 * dk + dv, dk))
    ):
        loads.append(pltpu.make_async_copy(w, wall.at[:, pl.ds(start, size)], w_sem.at[n]))
    for load in loads:
        load.start()
    dout_load = pltpu.make_async_copy(dout_in, dout_ref, w_sem.at[4])
    dout_load.start()
    x_copy(0, 0).start()

    barrier = pltpu.get_barrier_semaphore()
    for d in range(1, side):
        notify(barrier, "seq", first(d))
        notify(barrier, "seq", second(d))
    notify(barrier, "seq", partner)
    for to in target:
        notify(barrier, "tp", to)

    rows_at = lax.broadcasted_iota(jnp.int32, (CH, CH), 0)
    cols_at = lax.broadcasted_iota(jnp.int32, (CH, CH), 1)
    lower = (rows_at >= cols_at).astype(F32)
    lower_b = lower.astype(BF16)
    upper_b = (rows_at <= cols_at).astype(BF16)
    own_rate = rate_ref[...]

    state[...] = jnp.zeros_like(state)
    out_b[...] = jnp.zeros_like(out_b)
    r_send[...] = jnp.broadcast_to(own_rate, (PAD, dk))
    for load in loads:
        load.wait()
    for n in range(2):
        origin = seq_at(3 * n * (1 - core) + 2 * core, 3 * n * core + 2 * (1 - core), core)
        rows = pl.ds(pl.multiple_of(origin * depth, 16), depth)
        wmore[n] = wall[rows, 0:group].astype(F32)
    wown[...] = wall[pl.ds(pl.multiple_of(me * depth, 16), depth), 0:group].astype(F32)
    pl.semaphore_wait(barrier, 2 * side - 1 + tp - 1)
    for j in range(2):
        w_cross(j).start()
    for j in range(3):
        copy_r(j).start()
    for d in range(1, side):
        notify(met.at[0], "seq", first(d))
    dout_load.wait()
    for j in range(3):
        rows = pl.ds(pl.multiple_of(target[j] * chunk, chunk), chunk)
        d_send[j] = dout_ref[rows, :].astype(F32)

    def project_rows(out, slot, at, start):
        rows, half = slice(at, at + tile), width // 2
        cut = start + 2 * dk + dv
        out[:, : 2 * dk + dv] = mm(xbuf[slot, rows], wall[:, start:cut], NN)
        out[:, 2 * dk + dv :] = mm(
            xbuf[slot, rows, :half], wall[:half, cut : start + group], NN
        ) + mm(xbuf[slot, rows, half:], wall[half:, cut : start + group], NN)

    def post(out, t, kept, rate, total, dout_at, slope):
        proj, sq_all, w_all, s_all, m_all, cl_all = kept
        base = pl.multiple_of(t * tile, tile)
        proj[pl.ds(base, tile), :] = out[:, : 2 * dk + dv].astype(BF16)
        squashed = jax.nn.sigmoid(out[:, 2 * dk + dv :])
        sq_all[pl.ds(base, tile), :] = squashed
        for n in range(tile // CH):
            here = slice(n * CH, (n + 1) * CH)
            b = t * (tile // CH) + n
            within = tri_sum(lower_b, -rate * squashed[here])
            rows = pl.ds(pl.multiple_of(base + n * CH, CH), CH)
            w_all[rows, :] = within
            closing = within[CH - 1 : CH]
            cl_all[b] = jnp.broadcast_to(closing, (PAD, dk))
            query = out[here, :dk].astype(BF16).astype(F32)
            key = out[here, dk : 2 * dk].astype(BF16).astype(F32)
            value = out[here, 2 * dk : 2 * dk + dv].astype(BF16)
            query_scaled = (query * jnp.exp(within)).astype(BF16)
            key_closing = (key * jnp.exp(closing - within)).astype(BF16)
            entering = state[0]
            s_all[b] = entering
            state[0] = jnp.exp(closing) * entering + mm(value, key_closing, TN)
            fed = mm(dout_at(rows), query_scaled, TN)
            m_all[b] = fed
            if slope is not None:
                state[1] += jnp.exp(total) * fed
                total = total + slope * closing
        return total

    def own_dout(rows):
        return dout_ref[rows, :]

    def project(k, total):
        slot = lax.rem(k, 2)
        x_copy(k, slot).wait()

        @pl.when(k + 1 < pairs)
        def _():
            x_copy(k + 1, 1 - slot).start()

        for at, *event in EARLY:
            @pl.when(k == at)
            def _():
                gather(*event)

        project_rows(out_a, slot, 0, 0)
        total = post(
            out_b, jnp.maximum(2 * k - 1, 0), own, own_rate, total, own_dout,
            jnp.minimum(k, 1).astype(F32),
        )
        project_rows(out_b, slot, tile, 0)
        return post(out_a, 2 * k, own, own_rate, total, own_dout, 1.0)

    total = lax.fori_loop(0, pairs, project, jnp.zeros((1, dk), F32))
    pl.semaphore_wait(met.at[0], side - 1)
    notify(met.at[1], "seq", partner)
    total = post(out_b, 2 * pairs - 1, own, own_rate, total, own_dout, 1.0)
    x_copy(rank, 0).start()

    msg[:, 0:part, :] = state[0].reshape(seq, part, dk)
    msg[:, part : 2 * part, :] = state[1].reshape(seq, part, dk)
    msg[:, 2 * part :, :] = jnp.broadcast_to(jnp.exp(total)[None], (seq, PAD, dk))
    pl.semaphore_wait(met.at[1], 1)

    def enter_leave(kept, count):
        s_all, m_all, cl_all = kept[3:]

        def enter(b, so_far):
            s_all[b] = s_all[b] + jnp.exp(so_far) * edge[0]
            return so_far + cl_all[b, 0:1, :]

        def leave(n, carry):
            b = count - 1 - n
            fed = m_all[b]
            leaving = edge[1]
            m_all[b] = leaving
            edge[1] = jnp.exp(cl_all[b, 0:1, :]) * leaving + fed
            return carry

        lax.fori_loop(0, count, enter, jnp.zeros((1, dk), F32))
        lax.fori_loop(0, count, leave, 0)

    def grads(b, kept, rate, dout_at, whole):
        proj, sq_all, w_all, s_all, m_all, cl_all = kept
        rows = pl.ds(pl.multiple_of(b * CH, CH), CH)
        query = proj[rows, 0:dk].astype(F32)
        key = proj[rows, dk : 2 * dk].astype(F32)
        value = proj[rows, 2 * dk : 2 * dk + dv]
        within, squashed, dout = w_all[rows, :], sq_all[rows, :], dout_at(rows)
        closing = within[CH - 1 : CH]
        entering, leaving = s_all[b], m_all[b]
        grow, shrink, rest = jnp.exp(within), jnp.exp(-within), jnp.exp(closing - within)
        query_f, key_f, close_f = query * grow, key * shrink, key * rest
        query_s, key_s, close_s = query_f.astype(BF16), key_f.astype(BF16), close_f.astype(BF16)
        d_scores = (mm(dout, value, NT) * lower).astype(BF16)
        leaving_b = leaving.astype(BF16)
        d_query_s = mm(dout, entering.astype(BF16), NN) + mm(d_scores, key_s, NN)
        d_key_s = mm(d_scores, query_s, TN)
        d_close = mm(value, leaving_b, NN)
        at_close = d_close * close_f
        d_within = d_query_s * query_f - d_key_s * key_f - at_close
        d_closing = jnp.sum(at_close, axis=0, keepdims=True) + jnp.exp(closing) * jnp.sum(
            leaving * entering, axis=0, keepdims=True
        )
        d_gate = tri_sum(upper_b, d_within) + d_closing
        pre = d_gate * -rate * squashed * (1.0 - squashed)
        if not whole:
            return pre
        scores = (mm(query_s, key_s, NT) * lower).astype(BF16)
        d_query = d_query_s * grow
        d_key = d_key_s * shrink + d_close * rest
        d_value = mm(scores, dout, TN) + mm(close_s, leaving_b, NT)
        return d_query, d_key, d_value, pre

    bounds = ((0, dk), (dk, 2 * dk), (2 * dk, 2 * dk + dv), (2 * dk + dv, group))

    def unpack(j, b):
        start = slots[j] * group
        w_pair(j, b).wait_recv()

        def run(a, carry):
            for buffer, on in ((land, core), (landd, 1 - core)):
                origin = seq_at(a * (1 - on) + b * on, a * on + b * (1 - on), on)
                rows = pl.ds(pl.multiple_of(origin * depth, 16), depth)
                wall[rows, start : start + group] = buffer[j, b, a].astype(BF16)
            return carry

        lax.fori_loop(0, 4, run, 0)

    def near(j):
        start = slots[j] * group
        def dout_at(rows):
            return d_recv[j, rows, :].astype(BF16)

        def before():
            state[0] = jnp.zeros((dv, dk), F32)
            project_rows(out_a, 0, 0, start)
            project_rows(out_b, 0, tile, start)
            rate = r_recv[j, 0:1, :]
            post(out_a, 0, other, rate, None, dout_at, None)
            post(out_b, 1, other, rate, None, dout_at, None)

        def run(h, carry):
            rate = r_recv[j, 0:1, :]
            pair = [grads(2 * h + n, other, rate, dout_at, True) for n in range(2)]
            for n in range(2):
                rows = pl.ds(pl.multiple_of((2 * h + n) * CH, CH), CH)
                for (lo, hi), grad in zip(bounds, pair[n]):
                    gmat[rows, slots[j] * group + lo : slots[j] * group + hi] = grad.astype(BF16)
            return carry

        def after():
            for n in range(2):
                copy_st(j, n).wait_recv()
            edge[0] = st_recv[j, 0]
            edge[1] = st_recv[j, 1]
            enter_leave(other, each)
            lax.fori_loop(0, each // 2, run, 0)

        return before, after

    def arrived(j):
        copy_r(j).wait_recv()
        copy_d(j).wait_recv()

    def scatter(d):
        to = lax.rem(me + d, seq)
        return remote(msg.at[to], got.at[d], e1_s.at[d], e1_r.at[d], "seq", to)

    def collect(d):
        to = lax.rem(me + d, seq)
        return remote(rep.at[to], back.at[me], e2_s.at[d], e2_r.at[d], "seq", to)

    def start_all(copy):
        def run(d, carry):
            copy(d).start()
            return carry

        lax.fori_loop(1, seq, run, 0)

    def wait_all(copy):
        def run(d, carry):
            copy(d).wait()
            return carry

        lax.fori_loop(1, seq, run, 0)

    def fold_states(p, run):
        it = lax.rem(me + seq - p, seq)
        rep[p, 0:part, :] = run
        return got[it, pl.ds(2 * part, 1), :] * run + got[it, pl.ds(0, part), :]

    def fold_grads(n, run):
        p = seq - 1 - n
        it = lax.rem(me + seq - p, seq)
        rep[p, part:, :] = run
        return got[it, pl.ds(2 * part, 1), :] * run + got[it, pl.ds(part, part), :]

    def scatter_start():
        start_all(scatter)
        got[0] = msg[me]

    def fold():
        wait_all(scatter)
        lax.fori_loop(0, seq, fold_states, jnp.zeros((part, dk), F32))
        lax.fori_loop(0, seq, fold_grads, jnp.zeros((part, dk), F32))
        start_all(collect)
        back[me] = rep[me]

    def own_states():
        wait_all(collect)
        edge[0] = back[:, 0:part, :].reshape(dv, dk)
        edge[1] = back[:, part:, :].reshape(dv, dk)
        enter_leave(own, blocks)
        for j in range(3):
            copy_st(j, 0).start()
            copy_st(j, 1).start()

    def signal_of(b, pre):
        sig_ref[pl.ds(pl.multiple_of(b * CH, CH), CH), :] = pre * scale

    def home(h, carry):
        pair = [grads(rank * each + 2 * h + n, own, own_rate, own_dout, True) for n in range(2)]
        for n in range(2):
            i = 2 * h + n
            signal_of(rank * each + i, pair[n][3])
            rows = pl.ds(pl.multiple_of(i * CH, CH), CH)
            for (lo, hi), grad in zip(bounds, pair[n]):
                gmat[rows, lo:hi] = grad.astype(BF16)
        return carry

    def aside(i, carry):
        found = [grads(target[j] * each + i, own, own_rate, own_dout, False) for j in range(3)]
        for j in range(3):
            signal_of(target[j] * each + i, found[j])
        return carry

    def back_first(lo, hi):
        for n in range(lo, hi):
            cols = slice(n * step, (n + 1) * step)
            acc[n] = mm(gmat[:, 0 : 2 * group], wall[cols, 0 : 2 * group], NT)

    def back_next(lo, hi):
        for n in range(lo, hi):
            cols = slice(n * step, (n + 1) * step)
            acc[n] += mm(gmat[:, 2 * group :], wall[cols, 2 * group :], NT)

    def own_chunk():
        x_copy(rank, 0).wait()

    heads = [near(j) for j in range(3)]
    steps = {
        "scatter": scatter_start, "fold": fold, "states": own_states, "chunk": own_chunk,
        "home": lambda lo, hi: lax.fori_loop(lo, hi, home, 0),
        "aside": lambda lo, hi: lax.fori_loop(lo, hi, aside, 0),
        "before": lambda j: (arrived(j), heads[j][0]()),
        "after": lambda j: heads[j][1](),
        "back_first": back_first, "back_next": back_next,
        "gather": gather, "unpack": unpack,
    }
    for name, *args in PLAN:
        steps[name](*args)
    at = slots[2] * group
    for n in range(width // step):
        cols = slice(n * step, (n + 1) * step)
        grad_ref[:, cols] = (
            acc[n] + mm(gmat[:, at : at + group], wall[cols, at : at + group], NT)
        ).astype(BF16)

    for j in range(3):
        w_cross(j).wait_send()
        copy_r(j).wait_send()
        copy_d(j).wait_send()
        for n in range(2):
            copy_st(j, n).wait_send()
        for n in range(4):
            w_line(j, n).wait_send()
            w_pair(j, n).wait_send()
        for n in range(12):
            if j == 2 or n not in (8, 11):
                w_plane(j, n).wait_send()
        if j < 2:
            w_more(j, 0).wait_send()
            w_more(j, 1).wait_send()


EARLY = ((2, 0, 0), (2, 2, 6), (3, 1, 0), (3, 0, 8), (3, 1, 8))
PLAN = (
    ("scatter",), ("gather", 0, 1), ("gather", 0, 2), ("gather", 0, 7), ("gather", 1, 7),
    ("fold",), ("gather", 0, 3), ("gather", 0, 4), ("gather", 1, 1),
    ("chunk",), ("unpack", 0, 0),
    ("gather", 1, 2), ("states",), ("gather", 2, 7), ("home", 0, 1), ("gather", 1, 3),
    ("home", 1, 2), ("gather", 0, 5), ("gather", 2, 0),
    ("unpack", 0, 3), ("unpack", 0, 1), ("gather", 1, 4), ("unpack", 0, 2),
    ("before", 0), ("aside", 0, 1), ("gather", 2, 1), ("unpack", 1, 0), ("aside", 1, 2),
    ("gather", 1, 5), ("unpack", 1, 3), ("gather", 2, 2),
    ("after", 0), ("gather", 2, 3), ("unpack", 1, 1), ("unpack", 1, 2),
    ("before", 1), ("gather", 2, 4), ("after", 1), ("back_first", 0, 5), ("gather", 2, 5),
    ("back_next", 0, 5), ("aside", 2, 4),
    ("unpack", 2, 0), ("unpack", 2, 3), ("unpack", 2, 1), ("unpack", 2, 2),
    ("before", 2), ("after", 2),
)


def solution(mesh):
    seq, tp = mesh.shape["seq"], mesh.shape["tp"]

    def body(tokens, w_query, w_key, w_value, w_gate, gate_rate, out_grad):
        length, width = tokens.shape
        dk, dv = w_query.shape[1], w_value.shape[1]
        blocks, each = length // CH, length // CH // tp
        tile = 2 * CH
        group = 3 * dk + dv
        chunk = each * CH
        scale = 4.0 * math.sqrt(length * seq * dk / dv)
        depth, part = width // seq, dv // seq
        step = 512 if width % 512 == 0 else width
        hbm = pl.BlockSpec(memory_space=pl.ANY)
        vmem = pl.BlockSpec(memory_space=pltpu.VMEM)
        dma = pltpu.SemaphoreType.DMA
        return pl.pallas_call(
            functools.partial(kernel, seq, tp, dk, dv, tile, scale),
            out_shape=(
                pltpu.VMEM((chunk, width), BF16),
                pltpu.VMEM((length, dk), F32),
            ),
            in_specs=[hbm] * 5 + [vmem, hbm],
            out_specs=(vmem, vmem),
            scratch_shapes=[
                pltpu.VMEM((width, 3 * group), BF16),
                pltpu.VMEM((2, 2 * tile, width), BF16),
                pltpu.VMEM((tile, group), F32),
                pltpu.VMEM((tile, group), F32),
                pltpu.VMEM((length, dv), BF16),
                pltpu.VMEM((length, 2 * dk + dv), BF16),
                pltpu.VMEM((length, dk), F32),
                pltpu.VMEM((length, dk), F32),
                pltpu.VMEM((blocks, dv, dk), F32),
                pltpu.VMEM((blocks, dv, dk), F32),
                pltpu.VMEM((blocks, PAD, dk), F32),
                pltpu.VMEM((chunk, 2 * dk + dv), BF16),
                pltpu.VMEM((chunk, dk), F32),
                pltpu.VMEM((chunk, dk), F32),
                pltpu.VMEM((each, dv, dk), F32),
                pltpu.VMEM((each, dv, dk), F32),
                pltpu.VMEM((each, PAD, dk), F32),
                pltpu.VMEM((2, dv, dk), F32),
                pltpu.VMEM((seq, 2 * part + PAD, dk), F32),
                pltpu.VMEM((seq, 2 * part + PAD, dk), F32),
                pltpu.VMEM((seq, 2 * part, dk), F32),
                pltpu.VMEM((seq, 2 * part, dk), F32),
                pltpu.VMEM((2, dv, dk), F32),
                pltpu.VMEM((depth, group), F32),
                pltpu.VMEM((2, depth, group), F32),
                pltpu.VMEM((3, 4, 4, depth, group), F32),
                pltpu.VMEM((3, 4, 4, depth, group), F32),
                pltpu.VMEM((3, chunk, dv), F32),
                pltpu.VMEM((3, chunk, dv), F32),
                pltpu.VMEM((PAD, dk), F32),
                pltpu.VMEM((3, PAD, dk), F32),
                pltpu.VMEM((3, 2, dv, dk), F32),
                pltpu.VMEM((chunk, 3 * group), BF16),
                pltpu.VMEM((width // step, chunk, step), F32),
            ]
            + [dma((5,)), dma((2,))]
            + [dma((seq,))] * 4
            + [dma((3,))] * 2
            + [dma((2, 2))] * 2
            + [dma((3, 4))] * 2
            + [dma((3, 12))] * 2
            + [dma((3, 4))] * 2
            + [dma((3,))] * 4
            + [dma((3, 2))] * 2
            + [pltpu.SemaphoreType.REGULAR((2,))],
            compiler_params=pltpu.CompilerParams(
                collective_id=0, has_side_effects=True, vmem_limit_bytes=VMEM_LIMIT
            ),
        )(tokens, w_query, w_key, w_value, w_gate, gate_rate.reshape(1, dk), out_grad)

    placed = (
        P("seq", None),
        P(None, "tp"),
        P(None, "tp"),
        P(None, "tp"),
        P(None, "tp"),
        P("tp"),
        P("seq", "tp"),
    )
    return jax.shard_map(
        body,
        mesh=mesh,
        in_specs=placed,
        out_specs=(P(("seq", "tp"), None), P("seq", "tp")),
        check_vma=False,
    )
```

```python
import functools
import math

import jax
import jax.numpy as jnp
from jax import lax
from jax.experimental import pallas as pl
from jax.experimental.pallas import tpu as pltpu
from jax.sharding import PartitionSpec as P

CH = 128
PAD = 8
VMEM_LIMIT = 63_200_000
F32, BF16 = jnp.float32, jnp.bfloat16


def mm(left, right, dims):
    return lax.dot_general(left, right, (dims, ((), ())), preferred_element_type=F32)


NN = ((1,), (0,))
NT = ((1,), (1,))
TN = ((0,), (0,))


def tri_sum(triangle, rows):
    high = rows.astype(BF16)
    low = (rows - high.astype(F32)).astype(BF16)
    return mm(triangle, high, NN) + mm(triangle, low, NN)


def kernel(
    seq, tp, dk, dv, tile, scale,
    tok, wq, wk, wv, wg, rate_ref, dout_in,
    grad_ref, sig_ref,
    wall, xbuf, out_a, out_b, dout_ref, proj, sq_all, w_all, s_all, m_all, cl_all,
    proj_n, sq_n, w_n, s_n, m_n, cl_n, state, msg, got, rep, back, edge,
    wown, wmore, land, landd, d_send, d_recv, r_send, r_recv, st_recv, gmat, acc,
    w_sem, x_sem, e1_s, e1_r, e2_s, e2_r, y_s, y_r, ym_s, ym_r, p1_s, p1_r, p2_s, p2_r, dd_s, dd_r,
    do_s, do_r, ra_s, ra_r, st_s, st_r, met,
):
    me, rank = lax.axis_index("seq"), lax.axis_index("tp")
    length, width, group = dout_ref.shape[0], wall.shape[0], 3 * dk + dv
    blocks, pairs = length // CH, length // (2 * tile)
    each = blocks // tp
    chunk = each * CH
    step = 512 if width % 512 == 0 else width
    depth, part = width // seq, dv // seq
    side = math.isqrt(seq // 2)
    core, chip = lax.rem(me, 2), me // 2
    x_at, z_at = chip // side, lax.rem(chip, side)
    offs = (1, 3, 2)
    target = tuple(lax.rem(rank + tp - off, tp) for off in offs)
    slots = (1, 2, 1)
    own = (proj, sq_all, w_all, s_all, m_all, cl_all)
    other = (proj_n, sq_n, w_n, s_n, m_n, cl_n)

    def seq_at(dx, dz, on):
        return (lax.rem(x_at + dx, side) * side + lax.rem(z_at + dz, side)) * 2 + on

    def first(d):
        return seq_at((1 - core) * d, core * d, core)

    def second(d):
        return seq_at(core * d, (1 - core) * d, core)

    ahead, behind = (first(1), second(1)), (first(side - 1), second(side - 1))
    partner = me + 1 - 2 * core

    def remote(src, dst, send, recv, axis, to):
        return pltpu.make_async_remote_copy(
            src_ref=src, dst_ref=dst, send_sem=send, recv_sem=recv, device_id={axis: to},
            device_id_type=pl.DeviceIdType.MESH,
        )

    def notify(sem, axis, to):
        pl.semaphore_signal(
            sem, inc=1, device_id={axis: to}, device_id_type=pl.DeviceIdType.MESH
        )

    def w_cross(j):
        return remote(wown, land.at[j, 0, 0], y_s.at[j], y_r.at[j], "tp", target[j])

    def w_more(j, n):
        a = 3 * n
        return remote(
            wmore.at[n], land.at[j, 2, a], ym_s.at[j, n], ym_r.at[j, n], "tp", target[j]
        )

    def w_line(j, n):
        half = depth // 2
        if n == 0:
            a, b, to = land.at[j, 0, 0], land.at[j, 0, 3], ahead[0]
        elif n == 1:
            a, b, to = land.at[j, 0, 0], land.at[j, 0, 1], behind[0]
        elif n == 2:
            rows = pl.ds(0, half)
            a, b, to = land.at[j, 0, 3, rows], land.at[j, 0, 2, rows], ahead[0]
        else:
            rows = pl.ds(half, half)
            a, b, to = land.at[j, 0, 1, rows], land.at[j, 0, 2, rows], behind[0]
        return remote(a, b, p1_s.at[j, n], p1_r.at[j, n], "seq", to)

    def w_plane(j, n):
        a = n % 4
        if n < 4:
            src, dst, to = land.at[j, 0, a], land.at[j, 3, a], ahead[1]
        elif n < 8:
            src, dst, to = land.at[j, 0, a], land.at[j, 1, a], behind[1]
        elif a < 2:
            src, dst, to = land.at[j, 3, a], land.at[j, 2, a], ahead[1]
        else:
            src, dst, to = land.at[j, 1, a], land.at[j, 2, a], behind[1]
        return remote(src, dst, p2_s.at[j, n], p2_r.at[j, n], "seq", to)

    def w_pair(j, b):
        return remote(land.at[j, b], landd.at[j, b], dd_s.at[j, b], dd_r.at[j, b], "seq", partner)

    def gather(j, stage):
        if stage == 0:
            w_cross(j).wait_recv()
            w_line(j, 0).start()
            w_line(j, 1).start()
            w_plane(j, 0).start()
            w_plane(j, 4).start()
        elif stage == 1:
            for n in (0, 1):
                w_line(j, n).wait_recv()
                w_line(j, n + 2).start()
            for a in (3, 1):
                w_plane(j, a).start()
                w_plane(j, 4 + a).start()
        elif stage == 2:
            for n in (2, 3):
                w_line(j, n).wait_recv()
            w_plane(j, 2).start()
            w_plane(j, 6).start()
            w_pair(j, 0).start()
        elif stage == 3:
            for a in (0, 3):
                w_plane(j, a).wait_recv()
                w_plane(j, 4 + a).wait_recv()
                if j == 2:
                    w_plane(j, 8 + a).start()
        elif stage == 4:
            for a in (1, 2):
                w_plane(j, a).wait_recv()
                w_plane(j, 4 + a).wait_recv()
                w_plane(j, 8 + a).start()
            w_pair(j, 3).start()
            w_pair(j, 1).start()
        elif stage == 5:
            for n in range(2):
                if j == 2:
                    w_plane(j, 8 + 3 * n).wait_recv()
                else:
                    w_more(j, n).wait_recv()
                w_plane(j, 9 + n).wait_recv()
            w_pair(j, 2).start()
        elif stage == 8:
            w_more(j, 0).start()
            w_more(j, 1).start()
        elif stage == 6:
            w_cross(j).start()
        else:
            copy_d(j).start()

    def x_copy(k, slot):
        return pltpu.make_async_copy(
            tok.at[pl.ds(pl.multiple_of(k * 2 * tile, 2 * tile), 2 * tile), :], xbuf.at[slot],
            x_sem.at[slot],
        )

    def copy_d(j):
        return remote(d_send.at[j], d_recv.at[j], do_s.at[j], do_r.at[j], "tp", target[j])

    def copy_r(j):
        return remote(r_send, r_recv.at[j], ra_s.at[j], ra_r.at[j], "tp", target[j])

    def copy_st(j, n):
        source = (s_all.at[target[j] * each], m_all.at[target[j] * each + each - 1])[n]
        return remote(source, st_recv.at[j, n], st_s.at[j, n], st_r.at[j, n], "tp", target[j])

    loads = []
    for n, (w, start, size) in enumerate(
        ((wq, 0, dk), (wk, dk, dk), (wv, 2 * dk, dv), (wg, 2 * dk + dv, dk))
    ):
        loads.append(pltpu.make_async_copy(w, wall.at[:, pl.ds(start, size)], w_sem.at[n]))
    for load in loads:
        load.start()
    dout_load = pltpu.make_async_copy(dout_in, dout_ref, w_sem.at[4])
    dout_load.start()
    x_copy(0, 0).start()

    barrier = pltpu.get_barrier_semaphore()
    for d in range(1, side):
        notify(barrier, "seq", first(d))
        notify(barrier, "seq", second(d))
    notify(barrier, "seq", partner)
    for to in target:
        notify(barrier, "tp", to)

    rows_at = lax.broadcasted_iota(jnp.int32, (CH, CH), 0)
    cols_at = lax.broadcasted_iota(jnp.int32, (CH, CH), 1)
    lower = (rows_at >= cols_at).astype(F32)
    lower_b = lower.astype(BF16)
    upper_b = (rows_at <= cols_at).astype(BF16)
    own_rate = rate_ref[...]

    state[...] = jnp.zeros_like(state)
    out_b[...] = jnp.zeros_like(out_b)
    r_send[...] = jnp.broadcast_to(own_rate, (PAD, dk))
    for load in loads:
        load.wait()
    for n in range(2):
        origin = seq_at(3 * n * (1 - core) + 2 * core, 3 * n * core + 2 * (1 - core), core)
        rows = pl.ds(pl.multiple_of(origin * depth, 16), depth)
        wmore[n] = wall[rows, 0:group].astype(F32)
    wown[...] = wall[pl.ds(pl.multiple_of(me * depth, 16), depth), 0:group].astype(F32)
    pl.semaphore_wait(barrier, 2 * side - 1 + tp - 1)
    for j in range(2):
        w_cross(j).start()
    for j in range(3):
        copy_r(j).start()
    for d in range(1, side):
        notify(met.at[0], "seq", first(d))
    dout_load.wait()
    for j in range(3):
        rows = pl.ds(pl.multiple_of(target[j] * chunk, chunk), chunk)
        d_send[j] = dout_ref[rows, :].astype(F32)

    def project_rows(out, slot, at, start):
        rows, half = slice(at, at + tile), width // 2
        cut = start + 2 * dk + dv
        out[:, : 2 * dk + dv] = mm(xbuf[slot, rows], wall[:, start:cut], NN)
        out[:, 2 * dk + dv :] = mm(
            xbuf[slot, rows, :half], wall[:half, cut : start + group], NN
        ) + mm(xbuf[slot, rows, half:], wall[half:, cut : start + group], NN)

    def post(out, t, kept, rate, total, dout_at, slope):
        proj, sq_all, w_all, s_all, m_all, cl_all = kept
        base = pl.multiple_of(t * tile, tile)
        proj[pl.ds(base, tile), :] = out[:, : 2 * dk + dv].astype(BF16)
        squashed = jax.nn.sigmoid(out[:, 2 * dk + dv :])
        sq_all[pl.ds(base, tile), :] = squashed
        for n in range(tile // CH):
            here = slice(n * CH, (n + 1) * CH)
            b = t * (tile // CH) + n
            within = tri_sum(lower_b, -rate * squashed[here])
            rows = pl.ds(pl.multiple_of(base + n * CH, CH), CH)
            w_all[rows, :] = within
            closing = within[CH - 1 : CH]
            cl_all[b] = jnp.broadcast_to(closing, (PAD, dk))
            query = out[here, :dk].astype(BF16).astype(F32)
            key = out[here, dk : 2 * dk].astype(BF16).astype(F32)
            value = out[here, 2 * dk : 2 * dk + dv].astype(BF16)
            query_scaled = (query * jnp.exp(within)).astype(BF16)
            key_closing = (key * jnp.exp(closing - within)).astype(BF16)
            entering = state[0]
            s_all[b] = entering
            state[0] = jnp.exp(closing) * entering + mm(value, key_closing, TN)
            fed = mm(dout_at(rows), query_scaled, TN)
            m_all[b] = fed
            if slope is not None:
                state[1] += jnp.exp(total) * fed
                total = total + slope * closing
        return total

    def own_dout(rows):
        return dout_ref[rows, :]

    def project(k, total):
        slot = lax.rem(k, 2)
        x_copy(k, slot).wait()

        @pl.when(k + 1 < pairs)
        def _():
            x_copy(k + 1, 1 - slot).start()

        for at, *event in EARLY:
            @pl.when(k == at)
            def _():
                gather(*event)

        project_rows(out_a, slot, 0, 0)
        total = post(
            out_b, jnp.maximum(2 * k - 1, 0), own, own_rate, total, own_dout,
            jnp.minimum(k, 1).astype(F32),
        )
        project_rows(out_b, slot, tile, 0)
        return post(out_a, 2 * k, own, own_rate, total, own_dout, 1.0)

    total = lax.fori_loop(0, pairs, project, jnp.zeros((1, dk), F32))
    pl.semaphore_wait(met.at[0], side - 1)
    notify(met.at[1], "seq", partner)
    total = post(out_b, 2 * pairs - 1, own, own_rate, total, own_dout, 1.0)
    x_copy(rank, 0).start()

    msg[:, 0:part, :] = state[0].reshape(seq, part, dk)
    msg[:, part : 2 * part, :] = state[1].reshape(seq, part, dk)
    msg[:, 2 * part :, :] = jnp.broadcast_to(jnp.exp(total)[None], (seq, 1, dk))
    pl.semaphore_wait(met.at[1], 1)

    def enter_leave(kept, count):
        s_all, m_all, cl_all = kept[3:]

        def enter(b, so_far):
            s_all[b] = s_all[b] + jnp.exp(so_far) * edge[0]
            return so_far + cl_all[b, 0:1, :]

        def leave(n, carry):
            b = count - 1 - n
            fed = m_all[b]
            leaving = edge[1]
            m_all[b] = leaving
            edge[1] = jnp.exp(cl_all[b, 0:1, :]) * leaving + fed
            return carry

        lax.fori_loop(0, count, enter, jnp.zeros((1, dk), F32))
        lax.fori_loop(0, count, leave, 0)

    def grads(b, kept, rate, dout_at, whole):
        proj, sq_all, w_all, s_all, m_all, cl_all = kept
        rows = pl.ds(pl.multiple_of(b * CH, CH), CH)
        query = proj[rows, 0:dk].astype(F32)
        key = proj[rows, dk : 2 * dk].astype(F32)
        value = proj[rows, 2 * dk : 2 * dk + dv]
        within, squashed, dout = w_all[rows, :], sq_all[rows, :], dout_at(rows)
        closing = within[CH - 1 : CH]
        entering, leaving = s_all[b], m_all[b]
        grow, shrink, rest = jnp.exp(within), jnp.exp(-within), jnp.exp(closing - within)
        query_f, key_f, close_f = query * grow, key * shrink, key * rest
        query_s, key_s, close_s = query_f.astype(BF16), key_f.astype(BF16), close_f.astype(BF16)
        d_scores = (mm(dout, value, NT) * lower).astype(BF16)
        leaving_b = leaving.astype(BF16)
        d_query_s = mm(dout, entering.astype(BF16), NN) + mm(d_scores, key_s, NN)
        d_key_s = mm(d_scores, query_s, TN)
        d_close = mm(value, leaving_b, NN)
        at_close = d_close * close_f
        d_within = d_query_s * query_f - d_key_s * key_f - at_close
        d_closing = jnp.sum(at_close, axis=0, keepdims=True) + jnp.exp(closing) * jnp.sum(
            leaving * entering, axis=0, keepdims=True
        )
        d_gate = tri_sum(upper_b, d_within) + d_closing
        pre = d_gate * -rate * squashed * (1.0 - squashed)
        if not whole:
            return pre
        scores = (mm(query_s, key_s, NT) * lower).astype(BF16)
        d_query = d_query_s * grow
        d_key = d_key_s * shrink + d_close * rest
        d_value = mm(scores, dout, TN) + mm(close_s, leaving_b, NT)
        return d_query, d_key, d_value, pre

    bounds = ((0, dk), (dk, 2 * dk), (2 * dk, 2 * dk + dv), (2 * dk + dv, group))

    def unpack(j, b):
        start = slots[j] * group
        w_pair(j, b).wait_recv()

        def run(a, carry):
            for buffer, on in ((land, core), (landd, 1 - core)):
                origin = seq_at(a * (1 - on) + b * on, a * on + b * (1 - on), on)
                rows = pl.ds(pl.multiple_of(origin * depth, 16), depth)
                wall[rows, start : start + group] = buffer[j, b, a].astype(BF16)
            return carry

        lax.fori_loop(0, 4, run, 0)

    def near(j):
        start = slots[j] * group
        def dout_at(rows):
            return d_recv[j, rows, :].astype(BF16)

        def before():
            state[0] = jnp.zeros((dv, dk), F32)
            project_rows(out_a, 0, 0, start)
            project_rows(out_b, 0, tile, start)
            rate = r_recv[j, 0:1, :]
            post(out_a, 0, other, rate, None, dout_at, None)
            post(out_b, 1, other, rate, None, dout_at, None)

        def run(h, carry):
            rate = r_recv[j, 0:1, :]
            pair = [grads(2 * h + n, other, rate, dout_at, True) for n in range(2)]
            for n in range(2):
                rows = pl.ds(pl.multiple_of((2 * h + n) * CH, CH), CH)
                for (lo, hi), grad in zip(bounds, pair[n]):
                    gmat[rows, slots[j] * group + lo : slots[j] * group + hi] = grad.astype(BF16)
            return carry

        def after():
            for n in range(2):
                copy_st(j, n).wait_recv()
            edge[0] = st_recv[j, 0]
            edge[1] = st_recv[j, 1]
            enter_leave(other, each)
            lax.fori_loop(0, each // 2, run, 0)

        return before, after

    def arrived(j):
        copy_r(j).wait_recv()
        copy_d(j).wait_recv()

    def scatter(d):
        to = lax.rem(me + d, seq)
        return remote(msg.at[to], got.at[d], e1_s.at[d], e1_r.at[d], "seq", to)

    def collect(d):
        to = lax.rem(me + d, seq)
        return remote(rep.at[to], back.at[me], e2_s.at[d], e2_r.at[d], "seq", to)

    def start_all(copy):
        def run(d, carry):
            copy(d).start()
            return carry

        lax.fori_loop(1, seq, run, 0)

    def wait_all(copy):
        def run(d, carry):
            copy(d).wait()
            return carry

        lax.fori_loop(1, seq, run, 0)

    def fold_states(p, run):
        it = lax.rem(me + seq - p, seq)
        rep[p, 0:part, :] = run
        return got[it, pl.ds(2 * part, 1), :] * run + got[it, pl.ds(0, part), :]

    def fold_grads(n, run):
        p = seq - 1 - n
        it = lax.rem(me + seq - p, seq)
        rep[p, part:, :] = run
        return got[it, pl.ds(2 * part, 1), :] * run + got[it, pl.ds(part, part), :]

    def scatter_start():
        start_all(scatter)
        got[0] = msg[me]

    def fold():
        wait_all(scatter)
        lax.fori_loop(0, seq, fold_states, jnp.zeros((part, dk), F32))
        lax.fori_loop(0, seq, fold_grads, jnp.zeros((part, dk), F32))
        start_all(collect)
        back[me] = rep[me]

    def own_states():
        wait_all(collect)
        edge[0] = back[:, 0:part, :].reshape(dv, dk)
        edge[1] = back[:, part:, :].reshape(dv, dk)
        enter_leave(own, blocks)
        for j in range(2):
            copy_st(j, 0).start()
            copy_st(j, 1).start()

    def signal_of(b, pre):
        sig_ref[pl.ds(pl.multiple_of(b * CH, CH), CH), :] = pre * scale

    def home(h, carry):
        pair = [grads(rank * each + 2 * h + n, own, own_rate, own_dout, True) for n in range(2)]
        for n in range(2):
            i = 2 * h + n
            signal_of(rank * each + i, pair[n][3])
            rows = pl.ds(pl.multiple_of(i * CH, CH), CH)
            for (lo, hi), grad in zip(bounds, pair[n]):
                gmat[rows, lo:hi] = grad.astype(BF16)
        return carry

    def aside(i, carry):
        found = [grads(target[j] * each + i, own, own_rate, own_dout, False) for j in range(3)]
        for j in range(3):
            signal_of(target[j] * each + i, found[j])
        return carry

    def back_first(lo, hi):
        for n in range(lo, hi):
            cols = slice(n * step, (n + 1) * step)
            acc[n] = mm(gmat[:, 0 : 2 * group], wall[cols, 0 : 2 * group], NT)

    def back_next(lo, hi):
        for n in range(lo, hi):
            cols = slice(n * step, (n + 1) * step)
            acc[n] += mm(gmat[:, 2 * group :], wall[cols, 2 * group :], NT)

    def far_start():
        copy_st(2, 0).start()
        copy_st(2, 1).start()
        copy_d(2).start()

    def own_chunk():
        x_copy(rank, 0).wait()

    heads = [near(j) for j in range(3)]
    steps = {
        "scatter": scatter_start, "fold": fold, "states": own_states, "chunk": own_chunk,
        "home": lambda lo, hi: lax.fori_loop(lo, hi, home, 0),
        "aside": lambda lo, hi: lax.fori_loop(lo, hi, aside, 0),
        "before": lambda j: (arrived(j), heads[j][0]()),
        "after": lambda j: heads[j][1](),
        "back_first": back_first, "back_next": back_next,
        "gather": gather, "unpack": unpack, "far": far_start,
    }
    for name, *args in PLAN:
        steps[name](*args)
    at = slots[2] * group
    for n in range(width // step):
        cols = slice(n * step, (n + 1) * step)
        grad_ref[:, cols] = (
            acc[n] + mm(gmat[:, at : at + group], wall[cols, at : at + group], NT)
        ).astype(BF16)

    for j in range(3):
        w_cross(j).wait_send()
        copy_r(j).wait_send()
        copy_d(j).wait_send()
        for n in range(2):
            copy_st(j, n).wait_send()
        for n in range(4):
            w_line(j, n).wait_send()
            w_pair(j, n).wait_send()
        for n in range(12):
            if j == 2 or n not in (8, 11):
                w_plane(j, n).wait_send()
        if j < 2:
            w_more(j, 0).wait_send()
            w_more(j, 1).wait_send()


EARLY = ((2, 0, 0), (2, 2, 6), (3, 1, 0), (3, 0, 8), (3, 1, 8))
PLAN = (
    ("scatter",), ("gather", 0, 1), ("gather", 0, 2), ("gather", 0, 7), ("gather", 1, 7),
    ("fold",), ("gather", 0, 3), ("gather", 0, 4), ("gather", 1, 1),
    ("chunk",), ("unpack", 0, 0),
    ("gather", 1, 2), ("states",), ("home", 0, 1), ("gather", 1, 3),
    ("home", 1, 2), ("aside", 0, 1), ("gather", 0, 5), ("gather", 2, 0),
    ("unpack", 0, 3), ("unpack", 0, 1), ("aside", 1, 2), ("gather", 1, 4), ("unpack", 0, 2),
    ("before", 0), ("gather", 2, 1), ("far",), ("aside", 2, 3), ("unpack", 1, 0),
    ("gather", 1, 5), ("unpack", 1, 3), ("unpack", 1, 1), ("gather", 2, 2), ("after", 0),
    ("unpack", 1, 2), ("gather", 2, 3), ("before", 1), ("gather", 2, 4), ("after", 1),
    ("back_first", 0, 5), ("gather", 2, 5), ("back_next", 0, 5),
    ("unpack", 2, 0), ("unpack", 2, 3), ("unpack", 2, 1), ("aside", 3, 4), ("unpack", 2, 2),
    ("before", 2), ("after", 2),
)


def solution(mesh):
    seq, tp = mesh.shape["seq"], mesh.shape["tp"]

    def body(tokens, w_query, w_key, w_value, w_gate, gate_rate, out_grad):
        length, width = tokens.shape
        dk, dv = w_query.shape[1], w_value.shape[1]
        blocks, each = length // CH, length // CH // tp
        tile = 2 * CH
        group = 3 * dk + dv
        chunk = each * CH
        scale = 4.0 * math.sqrt(length * seq * dk / dv)
        depth, part = width // seq, dv // seq
        step = 512 if width % 512 == 0 else width
        hbm = pl.BlockSpec(memory_space=pl.ANY)
        vmem = pl.BlockSpec(memory_space=pltpu.VMEM)
        dma = pltpu.SemaphoreType.DMA
        return pl.pallas_call(
            functools.partial(kernel, seq, tp, dk, dv, tile, scale),
            out_shape=(
                pltpu.VMEM((chunk, width), BF16),
                pltpu.VMEM((length, dk), F32),
            ),
            in_specs=[hbm] * 5 + [vmem, hbm],
            out_specs=(vmem, vmem),
            scratch_shapes=[
                pltpu.VMEM((width, 3 * group), BF16),
                pltpu.VMEM((2, 2 * tile, width), BF16),
                pltpu.VMEM((tile, group), F32),
                pltpu.VMEM((tile, group), F32),
                pltpu.VMEM((length, dv), BF16),
                pltpu.VMEM((length, 2 * dk + dv), BF16),
                pltpu.VMEM((length, dk), F32),
                pltpu.VMEM((length, dk), F32),
                pltpu.VMEM((blocks, dv, dk), F32),
                pltpu.VMEM((blocks, dv, dk), F32),
                pltpu.VMEM((blocks, PAD, dk), F32),
                pltpu.VMEM((chunk, 2 * dk + dv), BF16),
                pltpu.VMEM((chunk, dk), F32),
                pltpu.VMEM((chunk, dk), F32),
                pltpu.VMEM((each, dv, dk), F32),
                pltpu.VMEM((each, dv, dk), F32),
                pltpu.VMEM((each, PAD, dk), F32),
                pltpu.VMEM((2, dv, dk), F32),
                pltpu.VMEM((seq, 2 * part + 1, dk), F32),
                pltpu.VMEM((seq, 2 * part + 1, dk), F32),
                pltpu.VMEM((seq, 2 * part, dk), F32),
                pltpu.VMEM((seq, 2 * part, dk), F32),
                pltpu.VMEM((2, dv, dk), F32),
                pltpu.VMEM((depth, group), F32),
                pltpu.VMEM((2, depth, group), F32),
                pltpu.VMEM((3, 4, 4, depth, group), F32),
                pltpu.VMEM((3, 4, 4, depth, group), F32),
                pltpu.VMEM((3, chunk, dv), F32),
                pltpu.VMEM((3, chunk, dv), F32),
                pltpu.VMEM((PAD, dk), F32),
                pltpu.VMEM((3, PAD, dk), F32),
                pltpu.VMEM((3, 2, dv, dk), F32),
                pltpu.VMEM((chunk, 3 * group), BF16),
                pltpu.VMEM((width // step, chunk, step), F32),
            ]
            + [dma((5,)), dma((2,))]
            + [dma((seq,))] * 4
            + [dma((3,))] * 2
            + [dma((2, 2))] * 2
            + [dma((3, 4))] * 2
            + [dma((3, 12))] * 2
            + [dma((3, 4))] * 2
            + [dma((3,))] * 4
            + [dma((3, 2))] * 2
            + [pltpu.SemaphoreType.REGULAR((2,))],
            compiler_params=pltpu.CompilerParams(
                collective_id=0, has_side_effects=True, vmem_limit_bytes=VMEM_LIMIT
            ),
        )(tokens, w_query, w_key, w_value, w_gate, gate_rate.reshape(1, dk), out_grad)

    placed = (
        P("seq", None),
        P(None, "tp"),
        P(None, "tp"),
        P(None, "tp"),
        P(None, "tp"),
        P("tp"),
        P("seq", "tp"),
    )
    return jax.shard_map(
        body,
        mesh=mesh,
        in_specs=placed,
        out_specs=(P(("seq", "tp"), None), P("seq", "tp")),
        check_vma=False,
    )
```
